8 devices in a mesh: dp: 1 (over z), cfg: 2 (over y), tp: 4 (over x, core).
Axes of the slice: x: 2, y: 2, z: 1, core: 2. Of those that a mesh axis runs over, the one named last changes fastest.
Arguments:
- hidden: bfloat16 [2, 4096, 1152], P(('dp', 'cfg'))
- caption: bfloat16 [2, 120, 1152], P(('dp', 'cfg'))
- cap_len: int32 [2], P(('dp', 'cfg'))
- t_block: bfloat16 [1, 6912], P('dp')
- t_embed: bfloat16 [1, 1152], P('dp')
- x_t: float32 [1, 128, 128, 4], P('dp')
- alpha_bar: float32 [1, 2], P('dp')
- mod_table: bfloat16 [2, 6, 1152], replicated
- w_qkv: bfloat16 [2, 1152, 3, 16, 72], P(None, None, None, 'tp')
- w_proj: bfloat16 [2, 16, 72, 1152], P(None, 'tp')
- w_cq: bfloat16 [2, 1152, 16, 72], P(None, None, 'tp')
- w_ckv: bfloat16 [2, 1152, 2, 16, 72], P(None, None, None, 'tp')
- w_cproj: bfloat16 [2, 16, 72, 1152], P(None, 'tp')
- w_fc1: bfloat16 [2, 1152, 4608], P(None, None, 'tp')
- w_fc2: bfloat16 [2, 4608, 1152], P(None, 'tp')
- final_table: bfloat16 [2, 1152], replicated
- w_out: bfloat16 [1152, 32], replicated
- b_out: bfloat16 [32], replicated
Outputs:
- output: float32 [1, 128, 128, 4], P('dp')
All inputs are finite; a program needn't handle non-finite values.
Results may differ from the reference program's by a relative error of at most 0.0120919.
Values are sent between devices in bfloat16 or wider.
A program may use at most 1 GiB of HBM per device.

```python
import jax
import jax.numpy as jnp
from jax import lax

BATCH_SIZE = 1
LATENT_SIDE = 128
MODEL_DIM = 1152
NUM_HEADS = 16
TEXT_LEN = 120
HIDDEN_FF = 4608

NUM_TOKENS = (LATENT_SIDE // 2) * (LATENT_SIDE // 2)
HEAD_DIM = MODEL_DIM // NUM_HEADS
GUIDANCE = 4.5
LN_EPS = 1e-6


def setup_inputs(seed: int = 0, part: int = 0) -> dict:
    part_keys = jax.random.split(jax.random.fold_in(jax.random.key(seed), part), 10)
    weight_keys = jax.random.split(jax.random.key(seed + 1), 11)
    total_rows = 2 * BATCH_SIZE
    common = jax.random.normal(part_keys[0], (total_rows, 1, MODEL_DIM), jnp.float32)
    tok_noise = jax.random.normal(part_keys[1], (total_rows, NUM_TOKENS, MODEL_DIM), jnp.float32)
    hidden = common + tok_noise
    cap_mean = jax.random.normal(part_keys[2], (total_rows, 1, MODEL_DIM), jnp.float32)
    caption = cap_mean + jax.random.normal(part_keys[3], (total_rows, TEXT_LEN, MODEL_DIM), jnp.float32)
    len_keys = jax.random.split(part_keys[4], 2)
    cond_len = jax.random.randint(len_keys[0], (BATCH_SIZE,), TEXT_LEN // 4, TEXT_LEN + 1)
    uncond_len = jax.random.randint(len_keys[1], (BATCH_SIZE,), 1, TEXT_LEN // 16 + 2)
    cap_len = jnp.concatenate([cond_len.at[0].set(TEXT_LEN), uncond_len]).astype(jnp.int32)
    t_block = 0.5 * jax.random.normal(part_keys[5], (BATCH_SIZE, 6 * MODEL_DIM), jnp.float32)
    t_embed = 0.5 * jax.random.normal(part_keys[6], (BATCH_SIZE, MODEL_DIM), jnp.float32)
    x_t = jax.random.normal(part_keys[7], (BATCH_SIZE, LATENT_SIDE, LATENT_SIDE, 4), jnp.float32)
    abar_t = jax.random.uniform(part_keys[8], (BATCH_SIZE,), jnp.float32, 0.15, 0.6)
    abar_gap = jax.random.uniform(part_keys[9], (BATCH_SIZE,), jnp.float32, 0.1, 0.3)
    alpha_bar = jnp.stack([abar_t, abar_t + abar_gap], axis=1)
    dim_scale = MODEL_DIM ** -0.5
    ff_scale = HIDDEN_FF ** -0.5
    mod_table = 0.5 * jax.random.normal(weight_keys[0], (2, 6, MODEL_DIM), jnp.float32)
    w_qkv = dim_scale * jax.random.normal(weight_keys[1], (2, MODEL_DIM, 3, NUM_HEADS, HEAD_DIM), jnp.float32)
    w_proj = dim_scale * jax.random.normal(weight_keys[2], (2, NUM_HEADS, HEAD_DIM, MODEL_DIM), jnp.float32)
    w_cq = dim_scale * jax.random.normal(weight_keys[3], (2, MODEL_DIM, NUM_HEADS, HEAD_DIM), jnp.float32)
    w_ckv = dim_scale * jax.random.normal(weight_keys[4], (2, MODEL_DIM, 2, NUM_HEADS, HEAD_DIM), jnp.float32)
    w_cproj = dim_scale * jax.random.normal(weight_keys[5], (2, NUM_HEADS, HEAD_DIM, MODEL_DIM), jnp.float32)
    w_fc1 = dim_scale * jax.random.normal(weight_keys[6], (2, MODEL_DIM, HIDDEN_FF), jnp.float32)
    w_fc2 = ff_scale * jax.random.normal(weight_keys[7], (2, HIDDEN_FF, MODEL_DIM), jnp.float32)
    final_table = 0.5 * jax.random.normal(weight_keys[8], (2, MODEL_DIM), jnp.float32)
    w_out = dim_scale * jax.random.normal(weight_keys[9], (MODEL_DIM, 32), jnp.float32)
    b_out = 0.3 * jax.random.normal(weight_keys[10], (32,), jnp.float32)
    return {
        'hidden': hidden.astype(jnp.bfloat16),
        'caption': caption.astype(jnp.bfloat16),
        'cap_len': cap_len,
        't_block': t_block.astype(jnp.bfloat16),
        't_embed': t_embed.astype(jnp.bfloat16),
        'x_t': x_t,
        'alpha_bar': alpha_bar,
        'mod_table': mod_table.astype(jnp.bfloat16),
        'w_qkv': w_qkv.astype(jnp.bfloat16),
        'w_proj': w_proj.astype(jnp.bfloat16),
        'w_cq': w_cq.astype(jnp.bfloat16),
        'w_ckv': w_ckv.astype(jnp.bfloat16),
        'w_cproj': w_cproj.astype(jnp.bfloat16),
        'w_fc1': w_fc1.astype(jnp.bfloat16),
        'w_fc2': w_fc2.astype(jnp.bfloat16),
        'final_table': final_table.astype(jnp.bfloat16),
        'w_out': w_out.astype(jnp.bfloat16),
        'b_out': b_out.astype(jnp.bfloat16),
    }


def layer_norm(values):
    mean_val = jnp.mean(values, axis=-1, keepdims=True)
    centered = values - mean_val
    variance = jnp.mean(centered * centered, axis=-1, keepdims=True)
    return centered * lax.rsqrt(variance + LN_EPS)


def attend(queries, key_vecs, values, key_mask):
    def one_head(head_in):
        q_head, k_head, v_head = head_in
        scores = jnp.dot(q_head, k_head.T, preferred_element_type=jnp.float32) * HEAD_DIM ** -0.5
        scores = jnp.where(key_mask[None, :], scores, -1e30)
        attn_prob = jax.nn.softmax(scores, axis=-1).astype(jnp.bfloat16)
        return jnp.dot(attn_prob, v_head, preferred_element_type=jnp.float32).astype(jnp.bfloat16)
    per_head = lax.map(one_head, (jnp.swapaxes(queries, 0, 1), jnp.swapaxes(key_vecs, 0, 1), jnp.swapaxes(values, 0, 1)))
    return jnp.swapaxes(per_head, 0, 1)


def block_row(residual, caption_row, key_mask, t_mods, layer_w):
    mod_tab, w_qkv, w_proj, w_cq, w_ckv, w_cproj, w_fc1, w_fc2 = layer_w
    mod_rows = mod_tab.astype(jnp.float32) + t_mods
    all_keys = jnp.ones((NUM_TOKENS,), jnp.bool_)
    attn_in = (layer_norm(residual) * (1.0 + mod_rows[1]) + mod_rows[0]).astype(jnp.bfloat16)
    qkv_out = jnp.dot(attn_in, w_qkv.reshape(MODEL_DIM, 3 * MODEL_DIM), preferred_element_type=jnp.float32)
    qkv_out = qkv_out.astype(jnp.bfloat16).reshape(NUM_TOKENS, 3, NUM_HEADS, HEAD_DIM)
    self_o = attend(qkv_out[:, 0], qkv_out[:, 1], qkv_out[:, 2], all_keys)
    self_proj = jnp.dot(self_o.reshape(NUM_TOKENS, MODEL_DIM), w_proj.reshape(MODEL_DIM, MODEL_DIM), preferred_element_type=jnp.float32).astype(jnp.bfloat16)
    residual = residual + mod_rows[2] * self_proj.astype(jnp.float32)
    cross_q = jnp.dot(residual.astype(jnp.bfloat16), w_cq.reshape(MODEL_DIM, MODEL_DIM), preferred_element_type=jnp.float32)
    cross_q = cross_q.astype(jnp.bfloat16).reshape(NUM_TOKENS, NUM_HEADS, HEAD_DIM)
    cross_kv = jnp.dot(caption_row, w_ckv.reshape(MODEL_DIM, 2 * MODEL_DIM), preferred_element_type=jnp.float32)
    cross_kv = cross_kv.astype(jnp.bfloat16).reshape(TEXT_LEN, 2, NUM_HEADS, HEAD_DIM)
    cross_o = attend(cross_q, cross_kv[:, 0], cross_kv[:, 1], key_mask)
    cross_proj = jnp.dot(cross_o.reshape(NUM_TOKENS, MODEL_DIM), w_cproj.reshape(MODEL_DIM, MODEL_DIM), preferred_element_type=jnp.float32).astype(jnp.bfloat16)
    residual = residual + cross_proj.astype(jnp.float32)
    mlp_in = (layer_norm(residual) * (1.0 + mod_rows[4]) + mod_rows[3]).astype(jnp.bfloat16)
    mlp_hidden = jax.nn.gelu(jnp.dot(mlp_in, w_fc1, preferred_element_type=jnp.float32), approximate=True).astype(jnp.bfloat16)
    mlp_out = jnp.dot(mlp_hidden, w_fc2, preferred_element_type=jnp.float32).astype(jnp.bfloat16)
    return residual + mod_rows[5] * mlp_out.astype(jnp.float32)


def reference(hidden, caption, cap_len, t_block, t_embed, x_t, alpha_bar, mod_table, w_qkv, w_proj, w_cq, w_ckv, w_cproj, w_fc1, w_fc2, final_table, w_out, b_out):
    t_rows = jnp.tile(t_block.astype(jnp.float32).reshape(BATCH_SIZE, 6, MODEL_DIM), (2, 1, 1))
    emb_rows = jnp.tile(t_embed.astype(jnp.float32), (2, 1))
    layer_ws = (mod_table, w_qkv, w_proj, w_cq, w_ckv, w_cproj, w_fc1, w_fc2)

    def per_row(row_in):
        hidden_row, caption_row, len_row, t_mods, emb_row = row_in
        key_mask = jnp.arange(TEXT_LEN) < len_row

        def layer_step(residual, layer_w):
            return block_row(residual, caption_row, key_mask, t_mods, layer_w), None

        residual, scan_out = lax.scan(layer_step, hidden_row.astype(jnp.float32), layer_ws)
        shift_scale = final_table.astype(jnp.float32) + emb_row[None, :]
        final_in = (layer_norm(residual) * (1.0 + shift_scale[1]) + shift_scale[0]).astype(jnp.bfloat16)
        out_tok = jnp.dot(final_in, w_out, preferred_element_type=jnp.float32) + b_out.astype(jnp.float32)
        grid_side = LATENT_SIDE // 2
        patches = out_tok.reshape(grid_side, grid_side, 2, 2, 8)[:, :, :, :, :4]
        return patches.transpose(0, 2, 1, 3, 4).reshape(LATENT_SIDE, LATENT_SIDE, 4)

    eps_rows = lax.map(per_row, (hidden, caption, cap_len, t_rows, emb_rows))
    eps_cond = eps_rows[:BATCH_SIZE]
    eps_uncond = eps_rows[BATCH_SIZE:]
    guided = eps_uncond + GUIDANCE * (eps_cond - eps_uncond)
    abar_t = alpha_bar[:, 0][:, None, None, None]
    abar_prev = alpha_bar[:, 1][:, None, None, None]
    x_zero = (x_t - jnp.sqrt(1.0 - abar_t) * guided) / jnp.sqrt(abar_t)
    return jnp.sqrt(abar_prev) * x_zero + jnp.sqrt(1.0 - abar_prev) * guided
```

```python
import functools
import math

import jax
import jax.numpy as jnp
from jax import lax
from jax.experimental import pallas as pl
from jax.experimental.pallas import tpu as pltpu
from jax.sharding import PartitionSpec as P

GUIDANCE = 4.5
LN_EPS = 1e-6
HD = 72
NH = 4
TP = 4
F32 = jnp.float32
BF16 = jnp.bfloat16
QK_SCALE = HD ** -0.5
QK_EXP2 = QK_SCALE * math.log2(math.e)
SAFE_EXP2 = 48.0
SAFE_V = 2.0 ** 40
VMEM = 60 * 2 ** 20
HBM = pl.BlockSpec(memory_space=pltpu.HBM)
MESH = pl.DeviceIdType.MESH
DOWN, ALONG = [dict(axis=axis, keepdims=True) for axis in range(2)]
PROJ, CQ, CPROJ, FC1, FC2A, FC2B = WEIGHTS = range(6)
SMALL = (PROJ, CQ, CPROJ)
PLACES = ('own', 'near', 'far_a', 'far_b', 'rest_a', 'rest_b')


def dot(a, b, dims='nn'):
    dims = {'nn': ((1,), (0,)), 'nt': ((1,), (1,)), 'tn': ((0,), (0,))}[dims]
    return lax.dot_general(a, b, (dims, ((), ())), preferred_element_type=F32)


def row(ref, i):
    return ref[pl.ds(i, 1)]


def layer_norm(values):
    mean_val = jnp.mean(values, **ALONG)
    centered = values - mean_val
    variance = jnp.mean(centered * centered, **ALONG)
    return centered * lax.rsqrt(variance + LN_EPS)


def where_am_i():
    t, y = lax.axis_index('tp'), lax.axis_index('cfg')
    return t, y, lax.rem(t, 2)


def target(kind):
    t, y, c = where_am_i()
    return {
        'core': {'tp': t + 1 - 2 * c, 'cfg': y},
        'x': {'tp': lax.rem(t + 2, 4), 'cfg': y},
        'diag': {'tp': 3 - t, 'cfg': y},
        'y': {'tp': t, 'cfg': 1 - y},
    }[kind]


def guarded(cond, fn):
    if cond == 'all':
        fn()
        return
    _, y, c = where_am_i()
    pl.when(c == y if cond == 'same' else c != y)(fn)


def receiver(kind, cond):
    if cond == 'all' or kind in ('x', 'diag'):
        return cond
    return 'diff' if cond == 'same' else 'same'


def greet():
    barrier = pltpu.get_barrier_semaphore()
    for kind in ('core', 'x', 'diag', 'y'):
        pl.semaphore_signal(barrier, inc=1, device_id=target(kind), device_id_type=MESH)
    pl.semaphore_wait(barrier, 4)


class Comm:
    def __init__(self, ops, refs, sems):
        self.ops, self.refs, self.sems = ops, refs, sems
        self.left = {op[1] for op in ops}

    def descriptor(self, i):
        src, dst, kind, cond = self.ops[i]
        return pltpu.make_async_remote_copy(
            src_ref=self.refs[src], dst_ref=self.refs[dst], send_sem=self.sems.at[0, i], recv_sem=self.sems.at[1, i],
            device_id=target(kind), device_id_type=MESH)

    def start(self, ops):
        for i, op in enumerate(self.ops):
            if op in ops:
                guarded(op[3], lambda: self.descriptor(i).start())

    def arrive(self, name):
        if name in self.left:
            self.left.remove(name)
            i = [op[1] for op in self.ops].index(name)
            guarded(receiver(*self.ops[i][2:]), lambda: self.descriptor(i).wait_recv())

    def finish(self):
        for i, op in enumerate(self.ops):
            guarded(op[3], lambda: self.descriptor(i).wait_send())
            self.arrive(op[1])


class Buffers:
    def __init__(self):
        self.arrays = {}

    def put(self, name, array, shape=(), index=()):
        self.arrays[name] = array, shape or array.shape, index

    def take(self, made, outs):
        for name, array in zip(made, outs):
            self.put(name, array)

    def plan(self, ops):
        made = [op[1] for op in ops]
        read = []
        for op in ops:
            if op[0] not in made and op[0] not in read:
                read.append(op[0])
        return read, made

    def shape(self, name, ops):
        for src, dst, _, _ in ops:
            if dst == name:
                return self.shape(src, ops)
        return self.arrays[name][1]

    def operands(self, names):
        return [self.arrays[n][0] for n in names]

    def bind(self, read, made, in_refs, out_refs):
        refs = {}
        for n, ref in zip(read, in_refs):
            index = self.arrays[n][2]
            refs[n] = ref.at[index] if index else ref
        refs.update(zip(made, out_refs))
        return refs


def comm_params(cid, n_ops):
    return dict(
        sems=pltpu.SemaphoreType.DMA((2, n_ops)),
        params=pltpu.CompilerParams(vmem_limit_bytes=VMEM, collective_id=cid, has_side_effects=True),
    )


def qkv(bufs, x, mods, w_rows, w_heads, layer, gather, ops, cid):
    d = x.shape[1]
    n = x.shape[0] * (TP if gather else 1)
    blk = n // TP
    piece = NH * HD
    moves = [('a', 'a1', 'core', 'all'), ('a', 'a2', 'x', 'all'), ('a2', 'a3', 'core', 'all')] if gather else []
    bufs.put('a', x)
    all_ops = moves + ops
    read, made = bufs.plan(all_ops)
    if 'a' not in read:
        read = ['a'] + read
    n_in = 4 + len(read)

    def body(*refs):
        mod_ref, wq_ref, wk_ref, wv_ref = refs[:4]
        q_ref, k_ref, v_ref, n_ref = refs[n_in:n_in + 4]
        named = bufs.bind(read, made, refs[4:n_in], refs[n_in + 4:n_in + 4 + len(made)])
        xbuf, wqv, wk, lsem, sems = refs[n_in + 4 + len(made):]
        comm = Comm(all_ops, named, sems)
        step = pl.program_id(0)
        t, y, c = where_am_i()
        owners = [t, t + 1 - 2 * c, lax.rem(t + 2, 4), 3 - t]

        def load(s):
            src = named[['a', 'a1', 'a2', 'a3'][s]] if gather else named['a'].at[pl.ds(owners[s] * blk, blk)]
            return pltpu.make_async_copy(src, xbuf.at[s % 2], lsem.at[s % 2])

        for s in range(TP):
            @pl.when(step == s)
            def _():
                if s == 0:
                    load(0).start()
                    greet()
                    wqv[0:piece] = wq_ref[...]
                    wqv[piece:2 * piece] = wv_ref[...]
                    for h in range(NH):
                        head = jnp.concatenate([wk_ref[h].astype(F32), jnp.zeros((128 - HD, d), F32)], axis=0)
                        wk[h * 128:(h + 1) * 128] = head.astype(BF16)
                    comm.start([op for op in all_ops if op not in moves[2:]])
                if gather:
                    if s:
                        comm.arrive('a%d' % s)
                    if s == 2:
                        comm.start(moves[2:])
                    if s:
                        load(s).start()
                elif s + 1 < TP:
                    load(s + 1).start()
                load(s).wait()

        x = xbuf[lax.rem(step, 2)]
        a = x
        if not gather:
            shift, scale = row(mod_ref, 6 * layer), row(mod_ref, 6 * layer + 1)
            a = (layer_norm(x.astype(F32)) * (1.0 + scale) + shift).astype(BF16)
        qv = dot(wqv[...], a, 'nt')
        q, v = qv[:piece], qv[piece:]
        norms = []
        for h in range(NH):
            qh = q[h * HD:(h + 1) * HD].astype(BF16).astype(F32)
            q_ref[h] = jnp.concatenate([qh, jnp.zeros((128 - HD, blk), F32)], axis=0).astype(BF16)
            norms.append(jnp.max(jnp.sum(qh * qh, **DOWN), **ALONG))
        kb = dot(a, wk[...], 'nt').astype(BF16)
        k_ref[...] = kb
        for h in range(NH):
            kh = kb[:, h * 128:(h + 1) * 128].astype(F32)
            norms.append(jnp.max(jnp.sum(kh * kh, **ALONG), **DOWN))
        for h in range(NH):
            v_ref[h] = v[h * HD:(h + 1) * HD].astype(BF16)
        norms.append(jnp.max(jnp.max(jnp.abs(v), **DOWN), **ALONG))
        n_ref[0] = jnp.concatenate([jnp.broadcast_to(m, (1, 128)) for m in norms] + [jnp.zeros((7, 128), F32)], axis=0)

        @pl.when(step == TP - 1)
        def _():
            comm.finish()

    extra = comm_params(cid, len(all_ops))
    out = pl.pallas_call(
        body,
        grid=(TP,),
        in_specs=[
            pl.BlockSpec(mods.shape, lambda i: (0, 0)),
            pl.BlockSpec((None, None, piece, d), lambda i: (layer, 0, 0, 0)),
            pl.BlockSpec((None, None, NH, HD, d), lambda i: (layer, 1, 0, 0, 0)),
            pl.BlockSpec((None, None, piece, d), lambda i: (layer, 2, 0, 0)),
        ] + [HBM] * len(read),
        out_specs=[
            pl.BlockSpec((NH, 128, blk), lambda i: (0, 0, i)),
            pl.BlockSpec((blk, NH * 128), lambda i: (i, 0)),
            pl.BlockSpec((NH, HD, blk), lambda i: (0, 0, i)),
            pl.BlockSpec((1, 16, 128), lambda i: (i, 0, 0)),
        ] + [HBM] * len(made),
        out_shape=[
            jax.ShapeDtypeStruct((NH, 128, n), BF16),
            jax.ShapeDtypeStruct((n, NH * 128), BF16),
            jax.ShapeDtypeStruct((NH, HD, n), BF16),
            jax.ShapeDtypeStruct((TP, 16, 128), F32),
        ] + [jax.ShapeDtypeStruct(bufs.shape(m, all_ops), BF16) for m in made],
        scratch_shapes=[
            pltpu.VMEM((2, blk, d), BF16), pltpu.VMEM((2 * piece, d), BF16), pltpu.VMEM((NH * 128, d), BF16),
            pltpu.SemaphoreType.DMA((2,)), extra['sems'],
        ],
        compiler_params=extra['params'],
        name='qkv_%d' % cid,
    )(mods, w_rows, w_heads, w_rows, *bufs.operands(read))
    bufs.take(made, out[4:])
    return out[:4]


def attention(bufs, q, k, v, first, ops, cid, bq=1024, bk=512):
    n = k.shape[0]
    own = n // TP
    per = own // bq
    read, made = bufs.plan(ops)
    steps = (NH, 2 * per)

    def body(*refs):
        q_ref, k_ref, v_ref = refs[:3]
        o_ref = refs[3 + len(read)]
        named = bufs.bind(read, made, refs[3:3 + len(read)], refs[4 + len(read):4 + len(read) + len(made)])
        comm = Comm(ops, named, refs[-1])
        head, block = pl.program_id(0), pl.program_id(1)

        @pl.when((head == 0) & (block == 0))
        def _():
            greet()
            comm.start(ops)

        def score(j):
            return dot(k_ref[j * bk:(j + 1) * bk], q_ref[0])

        s = score(0)
        total = jnp.zeros((8, bq), F32)
        acc = jnp.zeros((HD, bq), F32)
        for j in range(n // bk):
            if j + 1 < n // bk:
                ahead = score(j + 1)
            p = jnp.exp2(s * QK_EXP2)
            part = jnp.sum(p.reshape(bk // 8, 8, bq), axis=0)
            mix = dot(v_ref[0, :, j * bk:(j + 1) * bk], p.astype(BF16))
            total, acc = total + part, acc + mix
            s = ahead
        o_ref[0, 0] = (acc / jnp.sum(total, **DOWN)).astype(BF16)

        @pl.when((head == steps[0] - 1) & (block == steps[1] - 1))
        def _():
            comm.finish()

    extra = comm_params(cid, len(ops))
    out = pl.pallas_call(
        body,
        grid=steps,
        in_specs=[
            pl.BlockSpec((1, 128, bq), lambda h, i: (h, 0, first * per + i)),
            pl.BlockSpec((n, 128), lambda h, i: (0, h)),
            pl.BlockSpec((1, HD, n), lambda h, i: (h, 0, 0)),
        ] + [HBM] * len(read),
        out_specs=[pl.BlockSpec((1, 1, HD, bq), lambda h, i: (i // per, h, 0, i % per))] + [HBM] * len(made),
        out_shape=[jax.ShapeDtypeStruct((2, NH, HD, own), BF16)]
        + [jax.ShapeDtypeStruct(bufs.shape(m, ops), BF16) for m in made],
        scratch_shapes=[extra['sems']],
        compiler_params=extra['params'],
        name='attn_%d' % cid,
    )(q, k, v, *bufs.operands(read))
    bufs.take(made, out[1:])
    return out[0]


def repair_body(n_ref, q_hbm, k_hbm, v_hbm, o_hbm, out_hbm, q_ref, k_ref, v_ref, o_ref, sems, *, first):
    big = jnp.max(n_ref[...], axis=0)
    bound = jnp.max(jnp.sqrt(big[0:4]) * jnp.sqrt(big[4:8])) * QK_EXP2
    own = o_hbm.shape[3]
    bq = q_ref.shape[1]
    n = k_ref.shape[0]

    @pl.when(jnp.logical_not((bound < SAFE_EXP2) & (jnp.max(big[8:9]) < SAFE_V)))
    def _():
        @pl.loop(0, NH)
        def _(h):
            col = pl.multiple_of(h * 128, 128)
            ins = [pltpu.make_async_copy(k_hbm.at[:, pl.ds(col, 128)], k_ref, sems.at[0]),
                   pltpu.make_async_copy(v_hbm.at[h], v_ref, sems.at[1])]
            for cp in ins:
                cp.start()
            for cp in ins:
                cp.wait()

            @pl.loop(0, 2 * own // bq)
            def _(i):
                cp = pltpu.make_async_copy(q_hbm.at[h, :, pl.ds(pl.multiple_of(first * own + i * bq, bq), bq)], q_ref, sems.at[2])
                cp.start()
                cp.wait()

                def step(j, carry):
                    top, total, acc = carry
                    row = pl.multiple_of(j * bq, bq)
                    s = dot(k_ref[pl.ds(row, bq)], q_ref[...])
                    high = jnp.maximum(top, jnp.max(s, **DOWN))
                    p = jnp.exp2((s - high) * QK_EXP2)
                    shrink = jnp.exp2((top - high) * QK_EXP2)
                    mix = dot(v_ref[:, pl.ds(row, bq)], p.astype(BF16))
                    return high, total * shrink + jnp.sum(p, **DOWN), acc * shrink + mix

                start = (jnp.full((1, bq), -3e38, F32), jnp.zeros((1, bq), F32), jnp.zeros((HD, bq), F32))
                _, total, acc = lax.fori_loop(0, n // bq, step, start)
                o_ref[...] = (acc / total).astype(BF16)
                dst = out_hbm.at[i // (own // bq), h, :, pl.ds(pl.multiple_of((i % (own // bq)) * bq, bq), bq)]
                cp = pltpu.make_async_copy(o_ref, dst, sems.at[3])
                cp.start()
                cp.wait()


def repair(norms, q, k, v, o, first, bq=512):
    n = k.shape[0]
    return pl.pallas_call(
        functools.partial(repair_body, first=first),
        in_specs=[pl.BlockSpec(memory_space=pltpu.VMEM)] + [HBM] * 4,
        out_specs=HBM,
        out_shape=jax.ShapeDtypeStruct(o.shape, o.dtype),
        scratch_shapes=[
            pltpu.VMEM((128, bq), BF16), pltpu.VMEM((n, 128), BF16), pltpu.VMEM((HD, n), BF16), pltpu.VMEM((HD, bq), BF16),
            pltpu.SemaphoreType.DMA((4,)),
        ],
        input_output_aliases={4: 0},
        compiler_params=pltpu.CompilerParams(vmem_limit_bytes=VMEM),
        name='repair',
    )(norms, q, k, v, o)


def tail(bufs, cap_len, x, o_own, o_far, o_rest, mods, cross, w_out, b_out, layer, last, plan, cid, bt=512):
    d = x.shape[1]
    n = o_own.shape[2]
    piece = NH * HD
    ops = [('o1', 'o1_in', 'core', 'all')] + plan[0] + plan[1] + plan[2]
    made = [op[1] for op in ops[1:]]
    read = [m for m in [(p, layer, w) for p in PLACES for w in WEIGHTS] if m not in made]
    read += [op[0] for op in ops[1:] if op[0] not in read + made]
    n_vmem = 8
    n_in = n_vmem + 4 + len(read)
    n_out = 1 if last else 2

    def body(*refs):
        s_ref, mod_ref, c0, c1, c2, c3, wout_ref, bout_ref, x_hbm, oo, of, orr = refs[:n_vmem + 4]
        outs = refs[n_in:n_in + n_out]
        named = bufs.bind(read, made, refs[n_vmem + 4:n_in], refs[n_in + n_out:n_in + n_out + len(made)])
        scratch = refs[n_in + n_out + len(made):]
        if last:
            xs, ms, scratch = scratch[0], scratch[1], scratch[2:]
            x_in = xs
        else:
            xs, ms = outs
            x_in, scratch = scratch[0], scratch[1:]
        os, wp, wcq, wcp, w1, w2, part, heads, lsem, osem, sems = scratch
        named['o1'] = oo.at[1]
        named['o1_in'] = os.at[piece:2 * piece]
        comm = Comm(ops, named, sems)
        c_refs = (c0, c1, c2, c3)

        def place(w, r):
            if w in SMALL:
                return (wp, wcq, wcp)[w].at[r * piece:(r + 1) * piece]
            if w == FC1:
                return w1.at[r % 2]
            return w2.at[r % 2, 0:d // 2] if w == FC2A else w2.at[r % 2, d // 2:d]

        def copy(name, w, r):
            return pltpu.make_async_copy(named[(name, layer, w)], place(w, r), lsem.at[w, r])

        def fetch(w, r):
            if r < 2:
                copy(PLACES[r], w, r).start()
                return
            for cond, name in zip(('same', 'diff'), PLACES[2 * r - 2:2 * r]):
                comm.arrive((name, layer, w))
                guarded(cond, copy(name, w, r).start)

        def ready(w, r):
            copy(PLACES[0], w, r).wait()

        t, _, _ = where_am_i()
        x_from = x_hbm if last else x_hbm.at[pl.ds(t * n, n)]
        pieces = [(oo.at[0], os.at[0:piece]), (of, os.at[2 * piece:3 * piece]), (orr, os.at[3 * piece:4 * piece]), (x_from, x_in)]
        loads = [pltpu.make_async_copy(src, dst, osem.at[i]) for i, (src, dst) in enumerate(pieces)]
        for cp in loads:
            cp.start()
        greet()
        comm.start(ops[:1] + plan[0])
        for w in SMALL:
            for r in range(TP):
                fetch(w, r)
        for cp in loads:
            cp.wait()
        comm.arrive('o1_in')
        for w in SMALL:
            for r in range(TP):
                ready(w, r)
        for r in range(2):
            for w in (FC1, FC2A, FC2B):
                fetch(w, r)

        gate1, shift2, scale2, gate2, shift3, scale3 = [row(mod_ref, 6 * layer + i) for i in range(2, 8)]
        keys = lax.broadcasted_iota(jnp.int32, (128, bt), 0) < s_ref[0]

        @pl.loop(0, n // bt)
        def _(b):
            rows = pl.ds(pl.multiple_of(b * bt, bt), bt)
            y = dot(os[:, rows], wp[...], 'tn')
            x = x_in[rows, :].astype(F32) + gate1 * y.astype(BF16).astype(F32)
            q = dot(wcq[...], x.astype(BF16), 'nt')
            for r in range(TP):
                scores = []
                for h in range(NH):
                    row = (r * NH + h) * HD
                    s = dot(c_refs[r][h], q[row:row + HD].astype(BF16), 'tn') * QK_SCALE
                    scores.append(jnp.where(keys, s, -1e30))
                probs = [jnp.exp(s - jnp.max(s, **DOWN)) for s in scores]
                totals = [jnp.sum(p, **DOWN) for p in probs]
                mixes = [dot(c_refs[r][NH + h], probs[h].astype(BF16)) for h in range(NH)]
                mixes = [m / total for m, total in zip(mixes, totals)]
                heads[r * piece:(r + 1) * piece] = jnp.concatenate(mixes, axis=0).astype(BF16)
            z = dot(heads[...], wcp[...], 'tn')
            x = x + z.astype(BF16).astype(F32)
            xs[rows, :] = x
            ms[rows, :] = (layer_norm(x) * (1.0 + scale2) + shift2).astype(BF16)

        for op in plan[1]:
            comm.arrive(op[0])
        comm.start(plan[1])

        @pl.loop(0, TP)
        def _(r):
            slot = lax.rem(r, 2)
            for s in range(TP):
                @pl.when(r == s)
                def _():
                    for w in (FC1, FC2A, FC2B):
                        ready(w, s)

            @pl.loop(0, n // bt)
            def _(b):
                rows = pl.ds(pl.multiple_of(b * bt, bt), bt)
                m = ms[rows, :]
                cuts = ((0, 512), (512, d))
                us = [dot(m, w1[slot, :, lo:hi]) for lo, hi in cuts]
                sums = []
                for u, (lo, hi) in zip(us, cuts):
                    half = 0.5 * u
                    g = half + half * jnp.tanh(u * (GELU0 + GELU1 * (u * u)))
                    sums.append(dot(g.astype(BF16), w2[slot, lo:hi, :]))
                add = sums[0] + sums[1]

                @pl.when(r == 0)
                def _():
                    part[rows, :] = add

                @pl.when(r > 0)
                def _():
                    part[rows, :] += add

            @pl.when(r == 0)
            def _():
                fetch(FC1, 2)
                if last:
                    fetch(FC2A, 2)
                    fetch(FC2B, 2)

            @pl.when(r == 1)
            def _():
                for op in plan[2]:
                    comm.arrive(op[0])
                comm.start(plan[2])
                if not last:
                    fetch(FC2A, 2)
                    fetch(FC2B, 2)
                fetch(FC1, 3)
                fetch(FC2A, 3)
                if last:
                    fetch(FC2B, 3)

            if not last:
                @pl.when(r == 2)
                def _():
                    fetch(FC2B, 3)

        @pl.loop(0, n // bt)
        def _(b):
            rows = pl.ds(pl.multiple_of(b * bt, bt), bt)
            x = xs[rows, :] + gate2 * part[rows, :].astype(BF16).astype(F32)
            a = (layer_norm(x) * (1.0 + scale3) + shift3).astype(BF16)
            if last:
                outs[0][:, rows] = dot(wout_ref[...], a, 'nt') + bout_ref[:, 0:1]
            else:
                xs[rows, :] = x
                ms[rows, :] = a

        comm.finish()

    vm = pl.BlockSpec(memory_space=pltpu.VMEM)
    if last:
        out_shape = [jax.ShapeDtypeStruct((w_out.shape[0], n), F32)]
        scratch = [pltpu.VMEM((n, d), F32), pltpu.VMEM((n, d), BF16)]
    else:
        out_shape = [jax.ShapeDtypeStruct((n, d), F32), jax.ShapeDtypeStruct((n, d), BF16)]
        scratch = [pltpu.VMEM((n, d), BF16)]
    extra = comm_params(cid, len(ops))
    square = pltpu.VMEM((d, d), BF16)
    pair = pltpu.VMEM((2, d, d), BF16)
    of_layer = pl.BlockSpec((None, *cross[0].shape[1:]), lambda i: (layer, 0, 0, 0))
    out = pl.pallas_call(
        body,
        grid=(1,),
        in_specs=[pl.BlockSpec(memory_space=pltpu.SMEM), vm] + [of_layer] * TP + [vm, vm] + [HBM] * (4 + len(read)),
        out_specs=[vm] * n_out + [HBM] * len(made),
        out_shape=out_shape + [jax.ShapeDtypeStruct(bufs.shape(m, ops), BF16) for m in made],
        scratch_shapes=scratch + [
            pltpu.VMEM((d, n), BF16), square, square, square, pair, pair, pltpu.VMEM((n, d), F32), pltpu.VMEM((d, bt), BF16),
            pltpu.SemaphoreType.DMA((len(WEIGHTS), TP)), pltpu.SemaphoreType.DMA((TP,)), extra['sems'],
        ],
        compiler_params=extra['params'],
        name='tail_%d' % cid,
    )(cap_len, mods, *cross, w_out, b_out, x, o_own, o_far, o_rest, *bufs.operands(read))
    bufs.take(made, out[n_out:])
    return out[:n_out]


def split3(v):
    high = v.astype(BF16)
    rest = v - high.astype(F32)
    mid = rest.astype(BF16)
    return high, mid, (rest - mid.astype(F32)).astype(BF16)


def finish(tokens, x_t, alpha_bar, cid):
    total, lanes = x_t.shape
    own = total // TP
    peers = ('core', 'x', 'diag')

    def body(tok_ref, x_ref, ab_ref, out_ref, mine, other, sems):
        t, y, _ = where_am_i()
        greet()
        cols = lax.broadcasted_iota(jnp.int32, (lanes, 2 * lanes), 1)
        twice = 2 * lax.broadcasted_iota(jnp.int32, (lanes, 2 * lanes), 0)
        terms = []
        for q in range(2):
            rows = [tok_ref[16 * p + 8 * q:16 * p + 8 * q + 8, k * lanes:(k + 1) * lanes] for k in range(8) for p in range(2)]
            pick = (cols == twice + q).astype(F32).astype(BF16)
            for part in split3(jnp.concatenate(rows, axis=0)):
                terms.append(dot(part, pick))
        wide = sum(terms[1:], terms[0])
        for k in range(8):
            for odd in range(2):
                half = wide[16 * k:16 * k + 16, odd * lanes:(odd + 1) * lanes]
                mine[16 * k + 8 * odd:16 * k + 8 * odd + 8] = jnp.concatenate([half[0:4], half[8:12]], axis=0)
        swap = pltpu.make_async_remote_copy(
            src_ref=mine, dst_ref=other, send_sem=sems.at[0, 3], recv_sem=sems.at[1, 3],
            device_id=target('y'), device_id_type=MESH)
        swap.start()
        swap.wait()
        cond, uncond = jnp.where(y == 0, mine[...], other[...]), jnp.where(y == 0, other[...], mine[...])
        guided = uncond + GUIDANCE * (cond - uncond)
        abar_t, abar_prev = ab_ref[0:1, 0:1], ab_ref[0:1, 1:2]
        rows = pl.ds(pl.multiple_of(t * own, own), own)
        x_zero = (x_ref[rows] - jnp.sqrt(1.0 - abar_t) * guided) / jnp.sqrt(abar_t)
        out_ref[rows] = jnp.sqrt(abar_prev) * x_zero + jnp.sqrt(1.0 - abar_prev) * guided
        sends = [pltpu.make_async_remote_copy(
            src_ref=out_ref.at[rows], dst_ref=out_ref.at[rows], send_sem=sems.at[0, i], recv_sem=sems.at[1, i],
            device_id=target(kind), device_id_type=MESH) for i, kind in enumerate(peers)]
        for cp in sends:
            cp.start()
        for cp in sends:
            cp.wait()

    vm = pl.BlockSpec(memory_space=pltpu.VMEM)
    return pl.pallas_call(
        body,
        in_specs=[vm] * 3,
        out_specs=vm,
        out_shape=jax.ShapeDtypeStruct(x_t.shape, F32),
        scratch_shapes=[pltpu.VMEM((own, lanes), F32), pltpu.VMEM((own, lanes), F32), pltpu.SemaphoreType.DMA((2, 4))],
        compiler_params=pltpu.CompilerParams(collective_id=cid, has_side_effects=True),
        name='finish',
    )(tokens, x_t, alpha_bar)


GELU0 = math.sqrt(2.0 / math.pi)
GELU1 = GELU0 * 0.044715


def over_x(layer, ws):
    return [(('own', layer, w), ('far_a', layer, w), 'x', 'same') for w in ws]


def to_core(layer, ws):
    return [(('own', layer, w), ('near', layer, w), 'core', 'all') for w in ws]


def forward(layer, ws):
    return [op for w in ws for op in (
        (('far_a', layer, w), ('far_b', layer, w), 'y', 'same'), (('far_a', layer, w), ('rest_b', layer, w), 'core', 'same'))]


def hand_on(layer, ws):
    return [(('far_b', layer, w), ('rest_a', layer, w), 'core', 'diff') for w in ws]


def solution(mesh):
    row_spec = P(('dp', 'cfg'))
    part_spec = P('dp')
    tp1, tp2, tp3 = [P(*(None,) * i, 'tp') for i in range(1, 4)]
    in_specs = (row_spec, row_spec, row_spec, part_spec, part_spec, part_spec, part_spec, P(),
                tp3, tp1, tp2, tp3, tp1, tp2, tp1, P(), P(), P())

    def local_step(hidden, caption, cap_len, t_block, t_embed, x_t, alpha_bar, mod_table, w_qkv, w_proj, w_cq, w_ckv, w_cproj, w_fc1, w_fc2, final_table, w_out, b_out):
        n, d = hidden.shape[1:]
        own_n = n // TP
        layers = mod_table.shape[0]

        w_heads = w_qkv.transpose(0, 2, 3, 4, 1)
        w_rows = w_heads.reshape(layers, 3, NH * HD, d)
        by_rows = lambda w: w.reshape(layers, NH * HD, d)
        owned = (by_rows(w_proj), by_rows(w_cq.transpose(0, 2, 3, 1)), by_rows(w_cproj), w_fc1)
        bufs = Buffers()
        for layer in range(layers):
            for w, array in enumerate(owned):
                bufs.put(('own', layer, w), array, array.shape[1:], (layer,))
            for half in range(2):
                index = (layer, slice(half * d // 2, (half + 1) * d // 2))
                bufs.put(('own', layer, FC2A + half), w_fc2, (d // 2, d), index)

        base = jnp.concatenate([t_block.reshape(6, d), t_block.reshape(6, d), t_embed, t_embed])
        mods = jnp.concatenate([mod_table.reshape(6 * layers, d), final_table]).astype(F32) + base.astype(F32)
        bout = jnp.broadcast_to(b_out.astype(F32)[:, None], (b_out.shape[0], 128))

        cap = jnp.pad(caption[0], ((0, 128 - caption.shape[1]), (0, 0)))
        ckv_t = w_ckv.transpose(0, 2, 3, 4, 1).reshape(layers * 2 * NH * HD, d)
        ckv = dot(ckv_t, cap, 'nt').astype(BF16).reshape(layers, 2 * NH, HD, 128)
        bufs.put('c', ckv)

        plans = [
            (to_core(0, WEIGHTS) + over_x(0, SMALL) + [('c', 'c1', 'core', 'all')],
             over_x(0, [FC1]) + forward(0, SMALL) + [('c', 'c2', 'x', 'all')],
             over_x(0, [FC2A]) + forward(0, [FC1]) + hand_on(0, SMALL) + [('c2', 'c3', 'core', 'all')],
             (over_x(0, [FC2B]) + forward(0, [FC2A]) + hand_on(0, [FC1]) + over_x(1, [FC1, PROJ, CQ]) + to_core(1, WEIGHTS),
              forward(0, [FC2B]) + hand_on(0, [FC2A]), hand_on(0, [FC2B]))),
            (over_x(1, [CPROJ]) + forward(1, [PROJ, CQ, FC1]),
             over_x(1, [FC2A, FC2B]) + forward(1, [CPROJ]) + hand_on(1, [PROJ, CQ, FC1]),
             forward(1, [FC2A, FC2B]) + hand_on(1, [CPROJ]),
             (hand_on(1, [FC2A, FC2B]), [], [])),
        ]
        x = a = hidden[0]
        for layer in range(layers):
            p_qkv, p_other, p_own, p_tail = plans[layer]
            cid = 1 + 4 * layer
            q, k, v, norms = qkv(bufs, a, mods, w_rows, w_heads, layer, layer > 0, p_qkv, cid)
            o = attention(bufs, q, k, v, 2, p_other, cid + 1)
            o = repair(norms, q, k, v, o, 2).reshape(2, NH * HD, own_n)
            for i in range(2):
                bufs.put(('o', layer, i), o, o.shape[1:], (i,))
            send = [(('o', layer, i), ('o_in', layer, i), kind, 'all') for i, kind in enumerate(('x', 'diag'))]
            o = attention(bufs, q, k, v, 0, send + p_own, cid + 2)
            o = repair(norms, q, k, v, o, 0).reshape(2, NH * HD, own_n)
            o_far, o_rest = [bufs.arrays[('o_in', layer, i)][0] for i in range(2)]
            cross = [bufs.arrays[m][0] for m in ('c', 'c1', 'c2', 'c3')]
            out = tail(bufs, cap_len, x, o, o_far, o_rest, mods, cross, w_out.T, bout, layer, layer == layers - 1, p_tail, cid + 3)
            x, a = out[0], out[-1]
        pixels = x_t.transpose(0, 1, 3, 2).reshape(-1, x_t.shape[2])
        x_prev = finish(x, pixels, alpha_bar, cid + 4)
        return x_prev.reshape(1, x_t.shape[1], x_t.shape[3], x_t.shape[2]).transpose(0, 1, 3, 2)

    return jax.shard_map(local_step, mesh=mesh, in_specs=in_specs, out_specs=part_spec, check_vma=False)
```

```python
import functools
import math

import jax
import jax.numpy as jnp
from jax import lax
from jax.experimental import pallas as pl
from jax.experimental.pallas import tpu as pltpu
from jax.sharding import PartitionSpec as P

GUIDANCE = 4.5
LN_EPS = 1e-6
HD = 72
NH = 4
TP = 4
F32 = jnp.float32
BF16 = jnp.bfloat16
QK_SCALE = HD ** -0.5
QK_EXP2 = QK_SCALE * math.log2(math.e)
SAFE_EXP2 = 48.0
SAFE_V = 1e12
VMEM = 62914560
HBM = pl.BlockSpec(memory_space=pltpu.HBM)
MESH = pl.DeviceIdType.MESH
DOWN, ALONG = [dict(axis=axis, keepdims=True) for axis in range(2)]
PROJ, CQ, CPROJ, FC1, FC2A, FC2B = WEIGHTS = range(6)
SMALL = (PROJ, CQ, CPROJ)
PLACES = ('own', 'near', 'far_a', 'far_b', 'rest_a', 'rest_b')


def dot(a, b, dims='nn'):
    dims = {'nn': ((1,), (0,)), 'nt': ((1,), (1,)), 'tn': ((0,), (0,))}[dims]
    return lax.dot_general(a, b, (dims, ((), ())), preferred_element_type=F32)


def row(ref, i):
    return ref[pl.ds(i, 1)]


def layer_norm(values):
    mean_val = jnp.mean(values, **ALONG)
    centered = values - mean_val
    variance = jnp.mean(centered * centered, **ALONG)
    return centered * lax.rsqrt(variance + LN_EPS)


def where_am_i():
    t, y = lax.axis_index('tp'), lax.axis_index('cfg')
    return t, y, lax.rem(t, 2)


def target(kind):
    t, y, c = where_am_i()
    return {
        'core': {'tp': t + 1 - 2 * c, 'cfg': y},
        'x': {'tp': lax.rem(t + 2, 4), 'cfg': y},
        'diag': {'tp': 3 - t, 'cfg': y},
        'y': {'tp': t, 'cfg': 1 - y},
    }[kind]


def guarded(cond, fn):
    if cond == 'all':
        fn()
        return
    _, y, c = where_am_i()
    pl.when(c == y if cond == 'same' else c != y)(fn)


def receiver(kind, cond):
    if cond == 'all' or kind in ('x', 'diag'):
        return cond
    return 'diff' if cond == 'same' else 'same'


def greet():
    barrier = pltpu.get_barrier_semaphore()
    for kind in ('core', 'x', 'diag', 'y'):
        pl.semaphore_signal(barrier, inc=1, device_id=target(kind), device_id_type=MESH)
    pl.semaphore_wait(barrier, 4)


class Comm:
    def __init__(self, ops, refs, sems):
        self.ops, self.refs, self.sems = ops, refs, sems
        self.left = {op[1] for op in ops}

    def descriptor(self, i):
        src, dst, kind, cond = self.ops[i]
        return pltpu.make_async_remote_copy(
            src_ref=self.refs[src], dst_ref=self.refs[dst], send_sem=self.sems.at[0, i], recv_sem=self.sems.at[1, i],
            device_id=target(kind), device_id_type=MESH)

    def start(self, ops):
        for i, op in enumerate(self.ops):
            if op in ops:
                guarded(op[3], lambda: self.descriptor(i).start())

    def arrive(self, name):
        if name in self.left:
            self.left.remove(name)
            i = [op[1] for op in self.ops].index(name)
            guarded(receiver(*self.ops[i][2:]), lambda: self.descriptor(i).wait_recv())

    def finish(self):
        for i, op in enumerate(self.ops):
            guarded(op[3], lambda: self.descriptor(i).wait_send())
            self.arrive(op[1])


class Buffers:
    def __init__(self):
        self.arrays = {}

    def put(self, name, array, shape=(), index=()):
        self.arrays[name] = array, shape or array.shape, index

    def take(self, made, outs):
        for name, array in zip(made, outs):
            self.put(name, array)

    def plan(self, ops):
        made = [op[1] for op in ops]
        read = []
        for op in ops:
            if op[0] not in made and op[0] not in read:
                read.append(op[0])
        return read, made

    def shape(self, name, ops):
        for src, dst, _, _ in ops:
            if dst == name:
                return self.shape(src, ops)
        return self.arrays[name][1]

    def operands(self, names):
        return [self.arrays[n][0] for n in names]

    def bind(self, read, made, in_refs, out_refs):
        refs = {}
        for n, ref in zip(read, in_refs):
            index = self.arrays[n][2]
            refs[n] = ref.at[index] if index else ref
        refs.update(zip(made, out_refs))
        return refs


def comm_params(cid, n_ops):
    return dict(
        sems=pltpu.SemaphoreType.DMA((2, n_ops)),
        params=pltpu.CompilerParams(vmem_limit_bytes=VMEM, collective_id=cid, has_side_effects=True),
    )


HALVES = ('a00', 'a01', 'a10', 'a11', 'a20', 'a30', 'a21', 'a31')
TIGHT = HALVES[4:]


def qkv(bufs, x, mods, w_rows, w_heads, layer, gather, ops, cid):
    d = x.shape[1]
    n = x.shape[0] * (TP if gather else 1)
    blk = n // len(HALVES)
    piece = NH * HD
    moves = []
    if gather:
        bufs.put('mid', x, (blk // 2, d), (slice(blk // 2, blk),))
        bufs.put('high', x, (blk, d), (slice(blk, 2 * blk),))
        moves = [('mid', 'a2m', 'x', 'all'), ('high', 'a2h', 'x', 'all'), ('a', 'a1', 'core', 'all'),
                 ('a2l', 'a3l', 'core', 'all'), ('a2m', 'a3m', 'core', 'all'), ('a2h', 'a3h', 'core', 'all')]
    late = moves[4:]
    all_ops = moves + ops
    bufs.put('a', x)
    read, made = bufs.plan(all_ops)
    read = ['a'] + [name for name in read if name != 'a']
    n_in = 4 + len(read)

    def body(*refs):
        mod_ref, wq_ref, wk_ref, wv_ref = refs[:4]
        q_ref, k_ref, v_ref, n_ref = refs[n_in:n_in + 4]
        named = bufs.bind(read, made, refs[4:n_in], refs[n_in + 4:n_in + 4 + len(made)])
        xbuf, wqv, wk, lsem, sems = refs[n_in + 4 + len(made):]
        comm = Comm(all_ops, named, sems)
        step = pl.program_id(0)
        t, y, c = where_am_i()
        owners = [t, t + 1 - 2 * c, lax.rem(t + 2, 4), 3 - t]

        def sources(s):
            r, half = [int(digit) for digit in HALVES[s][1:]]
            if not gather:
                return [named['a'].at[pl.ds(owners[r] * 2 * blk + half * blk, blk)]]
            if r < 2:
                return [named[('a', 'a1')[r]].at[half * blk:half * blk + blk]]
            return [named['a%d%s' % (r, part)] for part in ('h' if half else 'lm')]

        def load(s):
            copies, at = [], 0
            for i, src in enumerate(sources(s)):
                dst = xbuf.at[s % 2, at:at + src.shape[0]]
                copies.append(pltpu.make_async_copy(src, dst, lsem.at[s % 2, i]))
                at += src.shape[0]
            return copies

        def begin(s):
            for name in {'a10': ('a1',), 'a20': ('a2m',), 'a30': ('a3l', 'a3m'), 'a21': ('a2h',), 'a31': ('a3h',)}.get(HALVES[s], ()):
                comm.arrive(name)
            for cp in load(s):
                cp.start()

        for s in range(len(HALVES)):
            @pl.when(step == s)
            def _():
                if s == 0:
                    begin(s)
                    greet()
                    comm.start([op for op in all_ops if op not in late])
                    wqv[0:piece] = wq_ref[...]
                    wqv[piece:2 * piece] = wv_ref[...]
                    for h in range(NH):
                        head = jnp.concatenate([wk_ref[h].astype(F32), jnp.zeros((128 - HD, d), F32)])
                        wk[h * 128:(h + 1) * 128] = head.astype(BF16)
                if gather and HALVES[s] in TIGHT:
                    begin(s)
                    comm.start([op for op in late if op[0] == {'a20': 'a2m', 'a21': 'a2h'}.get(HALVES[s])])
                for cp in load(s):
                    cp.wait()
                for name in HALVES[s + 1:s + 2]:
                    if not gather or name not in TIGHT:
                        begin(s + 1)

        x = xbuf[lax.rem(step, 2)]
        a = x
        if not gather:
            shift, scale = row(mod_ref, 6 * layer), row(mod_ref, 6 * layer + 1)
            a = (layer_norm(x.astype(F32)) * (1.0 + scale) + shift).astype(BF16)
        qv = dot(wqv[...], a, 'nt')
        q, v = qv[:piece], qv[piece:]
        norms = []
        for h in range(NH):
            qh = q[h * HD:(h + 1) * HD].astype(BF16).astype(F32)
            q_ref[h] = jnp.concatenate([qh, jnp.zeros((128 - HD, blk), F32)]).astype(BF16)
            norms.append(jnp.max(jnp.sum(qh * qh, **DOWN), **ALONG))
        kb = dot(a, wk[...], 'nt').astype(BF16)
        k_ref[...] = kb
        for h in range(NH):
            kh = kb[:, h * 128:(h + 1) * 128].astype(F32)
            norms.append(jnp.max(jnp.sum(kh * kh, **ALONG), **DOWN))
        for h in range(NH):
            v_ref[h] = v[h * HD:(h + 1) * HD].astype(BF16)
        norms.append(jnp.max(jnp.max(jnp.abs(v), **DOWN), **ALONG))
        n_ref[0] = jnp.concatenate([jnp.broadcast_to(m, (1, 128)) for m in norms] + [jnp.zeros((7, 128), F32)])

        @pl.when(step == len(HALVES) - 1)
        def _():
            comm.finish()

    def block(i):
        return i + jnp.where(i == 5, 1, 0) - jnp.where(i == 6, 1, 0)

    extra = comm_params(cid, len(all_ops))
    out = pl.pallas_call(
        body,
        grid=(len(HALVES),),
        in_specs=[
            pl.BlockSpec(mods.shape, lambda i: (0, 0)),
            pl.BlockSpec((None, None, piece, d), lambda i: (layer, 0, 0, 0)),
            pl.BlockSpec((None, None, NH, HD, d), lambda i: (layer, 1, 0, 0, 0)),
            pl.BlockSpec((None, None, piece, d), lambda i: (layer, 2, 0, 0)),
        ] + [HBM] * len(read),
        out_specs=[
            pl.BlockSpec((NH, 128, blk), lambda i: (0, 0, block(i))),
            pl.BlockSpec((blk, NH * 128), lambda i: (block(i), 0)),
            pl.BlockSpec((NH, HD, blk), lambda i: (0, 0, block(i))),
            pl.BlockSpec((1, 16, 128), lambda i: (i, 0, 0)),
        ] + [HBM] * len(made),
        out_shape=[
            jax.ShapeDtypeStruct((NH, 128, n), BF16),
            jax.ShapeDtypeStruct((n, NH * 128), BF16),
            jax.ShapeDtypeStruct((NH, HD, n), BF16),
            jax.ShapeDtypeStruct((len(HALVES), 16, 128), F32),
        ] + [jax.ShapeDtypeStruct(bufs.shape(m, all_ops), BF16) for m in made],
        scratch_shapes=[
            pltpu.VMEM((2, blk, d), BF16), pltpu.VMEM((2 * piece, d), BF16), pltpu.VMEM((NH * 128, d), BF16),
            pltpu.SemaphoreType.DMA((2, 2)), extra['sems'],
        ],
        compiler_params=extra['params'],
        name='qkv_%d' % cid,
    )(mods, w_rows, w_heads, w_rows, *bufs.operands(read))
    bufs.take(made, out[4:])
    return out[:4]


def attention(bufs, q, k, v, first, ops, cid, bq=1024, bk=512):
    n = k.shape[0]
    own = n // TP
    per = own // bq
    read, made = bufs.plan(ops)
    steps = (NH, 2 * per)

    def body(*refs):
        q_ref, k_ref, v_ref = refs[:3]
        o_ref = refs[3 + len(read)]
        named = bufs.bind(read, made, refs[3:3 + len(read)], refs[4 + len(read):4 + len(read) + len(made)])
        comm = Comm(ops, named, refs[-1])
        head, block = pl.program_id(0), pl.program_id(1)

        @pl.when((head == 0) & (block == 0))
        def _():
            greet()
            comm.start(ops)

        def score(j):
            return dot(k_ref[j * bk:(j + 1) * bk], q_ref[0])

        s = score(0)
        total = jnp.zeros((8, bq), F32)
        acc = jnp.zeros((HD, bq), F32)
        for j in range(n // bk):
            if j + 1 < n // bk:
                ahead = score(j + 1)
            p = jnp.exp2(s * QK_EXP2)
            part = jnp.sum(p.reshape(bk // 8, 8, bq), axis=0)
            mix = dot(v_ref[0, :, j * bk:(j + 1) * bk], p.astype(BF16))
            total, acc = total + part, acc + mix
            s = ahead
        o_ref[0, 0] = (acc / jnp.sum(total, **DOWN)).astype(BF16)

        @pl.when((head == steps[0] - 1) & (block == steps[1] - 1))
        def _():
            comm.finish()

    extra = comm_params(cid, len(ops))
    out = pl.pallas_call(
        body,
        grid=steps,
        in_specs=[
            pl.BlockSpec((1, 128, bq), lambda h, i: (h, 0, first * per + i)),
            pl.BlockSpec((n, 128), lambda h, i: (0, h)),
            pl.BlockSpec((1, HD, n), lambda h, i: (h, 0, 0)),
        ] + [HBM] * len(read),
        out_specs=[pl.BlockSpec((1, 1, HD, bq), lambda h, i: (i // per, h, 0, i % per))] + [HBM] * len(made),
        out_shape=[jax.ShapeDtypeStruct((2, NH, HD, own), BF16)]
        + [jax.ShapeDtypeStruct(bufs.shape(m, ops), BF16) for m in made],
        scratch_shapes=[extra['sems']],
        compiler_params=extra['params'],
        name='attn_%d' % cid,
    )(q, k, v, *bufs.operands(read))
    bufs.take(made, out[1:])
    return out[0]


def repair_body(n_ref, q_hbm, k_hbm, v_hbm, o_hbm, out_hbm, q_ref, k_ref, v_ref, o_ref, sems, *, first):
    big = jnp.max(n_ref[...], axis=0)
    bound = jnp.max(jnp.sqrt(big[0:4]) * jnp.sqrt(big[4:8])) * QK_EXP2
    own = o_hbm.shape[3]
    bq = q_ref.shape[1]
    n = k_ref.shape[0]

    @pl.when(jnp.logical_not((bound < SAFE_EXP2) & (jnp.max(big[8:9]) < SAFE_V)))
    def _():
        @pl.loop(0, NH)
        def _(h):
            col = pl.multiple_of(h * 128, 128)
            ins = [pltpu.make_async_copy(k_hbm.at[:, pl.ds(col, 128)], k_ref, sems.at[0]),
                   pltpu.make_async_copy(v_hbm.at[h], v_ref, sems.at[1])]
            for cp in ins:
                cp.start()
            for cp in ins:
                cp.wait()

            @pl.loop(0, 2 * own // bq)
            def _(i):
                cp = pltpu.make_async_copy(q_hbm.at[h, :, pl.ds(pl.multiple_of(first * own + i * bq, bq), bq)], q_ref, sems.at[2])
                cp.start()
                cp.wait()

                def step(j, carry):
                    top, total, acc = carry
                    row = pl.multiple_of(j * bq, bq)
                    s = dot(k_ref[pl.ds(row, bq)], q_ref[...])
                    high = jnp.maximum(top, jnp.max(s, **DOWN))
                    p = jnp.exp2((s - high) * QK_EXP2)
                    shrink = jnp.exp2((top - high) * QK_EXP2)
                    mix = dot(v_ref[:, pl.ds(row, bq)], p.astype(BF16))
                    return high, total * shrink + jnp.sum(p, **DOWN), acc * shrink + mix

                start = (jnp.full((1, bq), -3e38, F32), jnp.zeros((1, bq), F32), jnp.zeros((HD, bq), F32))
                _, total, acc = lax.fori_loop(0, n // bq, step, start)
                o_ref[...] = (acc / total).astype(BF16)
                dst = out_hbm.at[i // (own // bq), h, :, pl.ds(pl.multiple_of((i % (own // bq)) * bq, bq), bq)]
                cp = pltpu.make_async_copy(o_ref, dst, sems.at[3])
                cp.start()
                cp.wait()


def repair(norms, q, k, v, o, first, bq=512):
    n = k.shape[0]
    return pl.pallas_call(
        functools.partial(repair_body, first=first),
        in_specs=[pl.BlockSpec(memory_space=pltpu.VMEM)] + [HBM] * 4,
        out_specs=HBM,
        out_shape=jax.ShapeDtypeStruct(o.shape, o.dtype),
        scratch_shapes=[
            pltpu.VMEM((128, bq), BF16), pltpu.VMEM((n, 128), BF16), pltpu.VMEM((HD, n), BF16), pltpu.VMEM((HD, bq), BF16),
            pltpu.SemaphoreType.DMA((4,)),
        ],
        input_output_aliases={4: 0},
        compiler_params=pltpu.CompilerParams(vmem_limit_bytes=VMEM),
        name='repair',
    )(norms, q, k, v, o)


def tail(bufs, cap_len, x, o_own, o_far, o_rest, mods, cross, w_out, b_out, layer, last, plan, cid, bt=512, bs=512):
    d = x.shape[1]
    n = o_own.shape[2]
    piece = NH * HD
    ops = [('o1', 'o1_in', 'core', 'all')] + sum(plan, [])
    bufs.put('low', x, (bt // 2, d))
    made = [op[1] for op in ops[1:]]
    read = [m for m in [(p, layer, w) for p in PLACES for w in WEIGHTS] if m not in made]
    read += [op[0] for op in sum(plan[:3], []) if op[0] not in read + made]
    n_vmem = 8
    n_in = n_vmem + 4 + len(read)
    n_out = 1 if last else 2

    def body(*refs):
        s_ref, mod_ref, c0, c1, c2, c3, wout_ref, bout_ref, x_hbm, oo, of, orr = refs[:n_vmem + 4]
        outs = refs[n_in:n_in + n_out]
        named = bufs.bind(read, made, refs[n_vmem + 4:n_in], refs[n_in + n_out:n_in + n_out + len(made)])
        scratch = refs[n_in + n_out + len(made):]
        xs, ms, os, wp, wcq, wcp, w1, w2, part, heads, lsem, osem, sems = scratch[:13]
        x_in = xs if last else scratch[13]
        named['o1'] = oo.at[1]
        named['o1_in'] = os.at[piece:2 * piece]
        if not last:
            named['low'] = outs[1].at[0:bt // 2]
        comm = Comm(ops, named, sems)
        c_refs = (c0, c1, c2, c3)

        def place(w, r):
            if w in SMALL:
                return (wp, wcq, wcp)[w].at[r * piece:(r + 1) * piece]
            low = r % 2 * d
            if w == FC1:
                return w1.at[r // 2, :, low:low + d]
            low = r * d + d // 2 * (w == FC2B)
            return w2.at[low:low + d // 2]

        def copy(name, w, r):
            return pltpu.make_async_copy(named[(name, layer, w)], place(w, r), lsem.at[w, r])

        def fetch(w, r):
            if r < 2:
                copy(PLACES[r], w, r).start()
                return
            for cond, name in zip(('same', 'diff'), PLACES[2 * r - 2:2 * r]):
                comm.arrive((name, layer, w))
                guarded(cond, copy(name, w, r).start)

        def ready(w, r):
            copy(PLACES[0], w, r).wait()

        t, _, _ = where_am_i()
        x_from = x_hbm if last else x_hbm.at[pl.ds(t * n, n)]
        pieces = [(oo.at[0], os.at[0:piece]), (of, os.at[2 * piece:3 * piece]), (orr, os.at[3 * piece:4 * piece]), (x_from, x_in)]
        loads = [pltpu.make_async_copy(src, dst, osem.at[i, 0]) for i, (src, dst) in enumerate(pieces)]
        for cp in loads:
            cp.start()
        here = [(w, r) for w in SMALL for r in range(TP) if r < 2 or (PLACES[2 * r - 2], layer, w) not in made]
        for w, r in here:
            fetch(w, r)
        greet()
        comm.start(ops[:1] + plan[0])
        for w in SMALL:
            for r in range(TP):
                if (w, r) not in here:
                    fetch(w, r)
        for cp in loads:
            cp.wait()
        comm.arrive('o1_in')
        for w in (FC1, FC2A, FC2B):
            for r in range(2):
                fetch(w, r)

        gate1, shift2, scale2, gate2, shift3, scale3 = [row(mod_ref, 6 * layer + i) for i in range(2, 8)]
        keys = lax.broadcasted_iota(jnp.int32, (128, bs), 0) < s_ref[0]

        @pl.loop(0, n // bs)
        def _(b):
            rows = pl.ds(pl.multiple_of(b * bs, bs), bs)

            def first(w):
                @pl.when(b == 0)
                def _():
                    for r in range(TP):
                        ready(w, r)

            first(PROJ)
            y = dot(os[:, rows], wp[...], 'tn')
            x = x_in[rows, :].astype(F32) + gate1 * y.astype(BF16).astype(F32)
            first(CQ)

            @pl.when(b == n // bs - 1)
            def _():
                for op in plan[1]:
                    comm.arrive(op[0])
                comm.start(plan[1])

            q = dot(wcq[...], x.astype(BF16), 'nt')
            for r in range(TP):
                scores = []
                for h in range(NH):
                    row = (r * NH + h) * HD
                    s = dot(c_refs[r][h], q[row:row + HD].astype(BF16), 'tn') * QK_SCALE
                    scores.append(jnp.where(keys, s, -1e30))
                probs = [jnp.exp(s - jnp.max(s, **DOWN)) for s in scores]
                totals = [jnp.sum(p, **DOWN) for p in probs]
                mixes = [dot(c_refs[r][NH + h], probs[h].astype(BF16)) for h in range(NH)]
                mixes = [m / total for m, total in zip(mixes, totals)]
                heads[r * piece:(r + 1) * piece] = jnp.concatenate(mixes).astype(BF16)
            first(CPROJ)
            z = dot(heads[...], wcp[...], 'tn')
            x = x + z.astype(BF16).astype(F32)
            xs[rows, :] = x
            ms[rows, :] = (layer_norm(x) * (1.0 + scale2) + shift2).astype(BF16)

        for r in range(2, TP):
            fetch(FC1, r)
            fetch(FC2A, r)

        def store(b):
            rows = pl.ds(pl.multiple_of(b * bt, bt), bt)
            return [pltpu.make_async_copy(v.at[rows], out.at[rows], osem.at[TP + i, b]) for i, (v, out) in enumerate(zip((xs, ms), outs))]

        cut = 512
        cuts = [(lo, min(lo + cut, 2 * d)) for lo in range(0, 2 * d, cut)]

        @pl.loop(0, TP)
        def _(i):
            pair, b = i // 2, i % 2
            for p in range(2):
                @pl.when(i == 2 * p)
                def _():
                    for w in (FC1, FC2A, FC2B):
                        for r in range(2):
                            ready(w, 2 * p + r)

            rows = pl.ds(pl.multiple_of(b * bt, bt), bt)
            m = ms[rows, :]

            def up(j):
                return dot(m, w1[pair, :, cuts[j][0]:cuts[j][1]])

            u, add = up(0), jnp.zeros((bt, d), F32)
            for j, (lo, hi) in enumerate(cuts):
                if hi < 2 * d:
                    ahead = up(j + 1)
                half = 0.5 * u
                g = half + half * jnp.tanh(u * (GELU0 + GELU1 * (u * u)))
                add += dot(g.astype(BF16), w2[pl.ds(pl.multiple_of(pair * 2 * d + lo, 256), hi - lo), :])
                u = ahead

            @pl.when(pair == 0)
            def _():
                part[rows, :] = add

            @pl.when(i == 1)
            def _():
                for op in plan[2]:
                    comm.arrive(op[0])
                comm.start(plan[2])
                for r in range(2, TP):
                    fetch(FC2B, r)

            @pl.when(pair == 1)
            def _():
                x = xs[rows, :] + gate2 * (part[rows, :] + add).astype(BF16).astype(F32)
                a = (layer_norm(x) * (1.0 + scale3) + shift3).astype(BF16)
                if last:
                    outs[0][:, rows] = dot(wout_ref[...], a, 'nt') + bout_ref[:, 0:1]
                else:
                    xs[rows, :] = x
                    ms[rows, :] = a
                    for cp in store(b):
                        cp.start()

            if plan[3]:
                @pl.when(i == 2)
                def _():
                    store(0)[1].wait()
                    comm.start(plan[3])

        if not last:
            for cp in store(0)[:1] + store(1):
                cp.wait()
        comm.finish()

    vm = pl.BlockSpec(memory_space=pltpu.VMEM)
    results = [jax.ShapeDtypeStruct((w_out.shape[0], n), F32)]
    if not last:
        results = [jax.ShapeDtypeStruct((n, d), dtype) for dtype in (F32, BF16)]
    extra = comm_params(cid, len(ops))
    square = pltpu.VMEM((d, d), BF16)
    of_layer = pl.BlockSpec((None, *cross[0].shape[1:]), lambda i: (layer, 0, 0, 0))
    out = pl.pallas_call(
        body,
        grid=(1,),
        in_specs=[pl.BlockSpec(memory_space=pltpu.SMEM), vm, of_layer] + [vm] * (TP + 1) + [HBM] * (4 + len(read)),
        out_specs=[vm if last else HBM] * n_out + [HBM] * len(made),
        out_shape=results + [jax.ShapeDtypeStruct(bufs.shape(m, ops), BF16) for m in made],
        scratch_shapes=[
            pltpu.VMEM((n, d), F32), pltpu.VMEM((n, d), BF16), pltpu.VMEM((d, n), BF16), square, square, square, pltpu.VMEM((2, d, 2 * d), BF16), pltpu.VMEM((TP * d, d), BF16), pltpu.VMEM((n, d), F32), pltpu.VMEM((d, bs), BF16),
            pltpu.SemaphoreType.DMA((len(WEIGHTS), TP)), pltpu.SemaphoreType.DMA((TP + 2, 2)), extra['sems'],
        ] + [pltpu.VMEM((n, d), BF16)] * (not last),
        compiler_params=extra['params'],
        name='tail_%d' % cid,
    )(cap_len, mods, *cross, w_out, b_out, x, o_own, o_far, o_rest, *bufs.operands(read))
    bufs.take(made, out[n_out:])
    return out[:n_out]


def split3(v):
    high = v.astype(BF16)
    rest = v - high.astype(F32)
    mid = rest.astype(BF16)
    return high, mid, (rest - mid.astype(F32)).astype(BF16)


def finish(tokens, x_t, alpha_bar, cid):
    total, lanes = x_t.shape
    own = total // TP
    peers = ('core', 'x', 'diag')

    def body(tok_ref, x_ref, ab_ref, out_ref, mine, other, sems):
        t, y, _ = where_am_i()
        greet()
        cols = lax.broadcasted_iota(jnp.int32, (lanes, 2 * lanes), 1)
        twice = 2 * lax.broadcasted_iota(jnp.int32, (lanes, 2 * lanes), 0)
        terms = []
        for q in range(2):
            rows = [tok_ref[16 * p + 8 * q:16 * p + 8 * q + 8, k * lanes:(k + 1) * lanes] for k in range(8) for p in range(2)]
            pick = (cols == twice + q).astype(F32).astype(BF16)
            for part in split3(jnp.concatenate(rows)):
                terms.append(dot(part, pick))
        wide = sum(terms[1:], terms[0])
        for k in range(8):
            for odd in range(2):
                half = wide[16 * k:16 * k + 16, odd * lanes:(odd + 1) * lanes]
                mine[16 * k + 8 * odd:16 * k + 8 * odd + 8] = jnp.concatenate([half[0:4], half[8:12]])
        swap = pltpu.make_async_remote_copy(
            src_ref=mine, dst_ref=other, send_sem=sems.at[0, 3], recv_sem=sems.at[1, 3],
            device_id=target('y'), device_id_type=MESH)
        swap.start()
        swap.wait()
        first, pair = y == 0, (mine[...], other[...])
        cond, uncond = jnp.where(first, *pair), jnp.where(first, *pair[::-1])
        guided = uncond + GUIDANCE * (cond - uncond)
        abar_t, abar_prev = ab_ref[:, :1], ab_ref[:, 1:]
        rows = pl.ds(pl.multiple_of(t * own, own), own)
        x_zero = (x_ref[rows] - jnp.sqrt(1.0 - abar_t) * guided) / jnp.sqrt(abar_t)
        out_ref[rows] = jnp.sqrt(abar_prev) * x_zero + jnp.sqrt(1.0 - abar_prev) * guided
        sends = [pltpu.make_async_remote_copy(
            src_ref=out_ref.at[rows], dst_ref=out_ref.at[rows], send_sem=sems.at[0, i], recv_sem=sems.at[1, i],
            device_id=target(kind), device_id_type=MESH) for i, kind in enumerate(peers)]
        for cp in sends:
            cp.start()
        for cp in sends:
            cp.wait()

    vm = pl.BlockSpec(memory_space=pltpu.VMEM)
    return pl.pallas_call(
        body,
        in_specs=[vm] * 3,
        out_specs=vm,
        out_shape=jax.ShapeDtypeStruct(x_t.shape, F32),
        scratch_shapes=[pltpu.VMEM((own, lanes), F32)] * 2 + [pltpu.SemaphoreType.DMA((2, 4))],
        compiler_params=pltpu.CompilerParams(collective_id=cid, has_side_effects=True),
        name='finish',
    )(tokens, x_t, alpha_bar)


GELU0 = math.sqrt(2.0 / math.pi)
GELU1 = GELU0 * 0.044715


def over_x(layer, ws):
    return [(('own', layer, w), ('far_a', layer, w), 'x', 'same') for w in ws]


def to_core(layer, ws):
    return [(('own', layer, w), ('near', layer, w), 'core', 'all') for w in ws]


def forward(layer, ws):
    return [op for w in ws for op in (
        (('far_a', layer, w), ('far_b', layer, w), 'y', 'same'), (('far_a', layer, w), ('rest_b', layer, w), 'core', 'same'))]


def hand_on(layer, ws):
    return [(('far_b', layer, w), ('rest_a', layer, w), 'core', 'diff') for w in ws]


def share(layer):
    return [(('c', 0, layer), ('c', r, layer), kind, 'all') for r, kind in ((1, 'core'), (2, 'x'))]


def share_on(layer):
    return [(('c', 2, layer), ('c', 3, layer), 'core', 'all')]


def solution(mesh):
    row_spec = P(('dp', 'cfg'))
    part_spec = P('dp')
    tp1, tp2, tp3 = [P(*(None,) * i, 'tp') for i in range(1, 4)]
    in_specs = (row_spec, row_spec, row_spec, part_spec, part_spec, part_spec, part_spec, P(),
                tp3, tp1, tp2, tp3, tp1, tp2, tp1, P(), P(), P())

    def local_step(hidden, caption, cap_len, t_block, t_embed, x_t, alpha_bar, mod_table, w_qkv, w_proj, w_cq, w_ckv, w_cproj, w_fc1, w_fc2, final_table, w_out, b_out):
        n, d = hidden.shape[1:]
        own_n = n // TP
        layers = mod_table.shape[0]

        w_heads = w_qkv.transpose(0, 2, 3, 4, 1)
        w_rows = w_heads.reshape(layers, 3, NH * HD, d)
        by_rows = lambda w: w.reshape(layers, NH * HD, d)
        owned = (by_rows(w_proj), by_rows(w_cq.transpose(0, 2, 3, 1)), by_rows(w_cproj), w_fc1)
        bufs = Buffers()
        for layer in range(layers):
            for w, array in enumerate(owned):
                bufs.put(('own', layer, w), array, array.shape[1:], (layer,))
            for half in range(2):
                index = (layer, slice(half * d // 2, (half + 1) * d // 2))
                bufs.put(('own', layer, FC2A + half), w_fc2, (d // 2, d), index)

        base = jnp.concatenate([t_block.reshape(6, d), t_block.reshape(6, d), t_embed, t_embed])
        mods = jnp.concatenate([mod_table.reshape(6 * layers, d), final_table]).astype(F32) + base.astype(F32)
        bout = jnp.broadcast_to(b_out.astype(F32)[:, None], (b_out.shape[0], 128))

        cap = jnp.pad(caption[0], ((0, 128 - caption.shape[1]), (0, 0)))
        ckv_t = w_ckv.transpose(0, 2, 3, 4, 1).reshape(layers * 2 * NH * HD, d)
        ckv = dot(ckv_t, cap, 'nt').astype(BF16).reshape(layers, 2 * NH, HD, 128)
        for layer in range(layers):
            bufs.put(('c', 0, layer), ckv, ckv.shape[1:], (layer,))

        plans = [
            (to_core(0, WEIGHTS) + over_x(0, SMALL) + share(0),
             over_x(0, [FC1]) + over_x(1, [PROJ]) + forward(0, SMALL) + share_on(0),
             over_x(0, [FC2A]) + forward(0, [FC1]) + forward(1, [PROJ]) + hand_on(0, SMALL),
             (over_x(0, [FC2B]) + forward(0, [FC2A]) + hand_on(0, [FC1]) + hand_on(1, [PROJ]) + over_x(1, [FC1]) + to_core(1, WEIGHTS),
              forward(0, [FC2B]) + hand_on(0, [FC2A]), hand_on(0, [FC2B]),
              [('low', 'a2l', 'x', 'all')])),
            (forward(1, [FC1]),
             over_x(1, [CQ, CPROJ, FC2A]) + hand_on(1, [FC1]) + share(1),
             forward(1, [CQ, CPROJ, FC2A]) + share_on(1),
             (hand_on(1, [CQ, CPROJ, FC2A]) + over_x(1, [FC2B]), forward(1, [FC2B]), hand_on(1, [FC2B]), [])),
        ]
        x = a = hidden[0]
        for layer in range(layers):
            p_qkv, p_other, p_own, p_tail = plans[layer]
            cid = 1 + 4 * layer
            q, k, v, norms = qkv(bufs, a, mods, w_rows, w_heads, layer, layer > 0, p_qkv, cid)
            o = attention(bufs, q, k, v, 2, p_other, cid + 1)
            o = repair(norms, q, k, v, o, 2).reshape(2, NH * HD, own_n)
            for i in range(2):
                bufs.put(('o', layer, i), o, o.shape[1:], (i,))
            send = [(('o', layer, i), ('o_in', layer, i), kind, 'all') for i, kind in enumerate(('x', 'diag'))]
            o = attention(bufs, q, k, v, 0, send + p_own, cid + 2)
            o = repair(norms, q, k, v, o, 0).reshape(2, NH * HD, own_n)
            o_far, o_rest = [bufs.arrays[('o_in', layer, i)][0] for i in range(2)]
            cross = [bufs.arrays[('c', r, layer)][0] for r in range(TP)]
            out = tail(bufs, cap_len, x, o, o_far, o_rest, mods, cross, w_out.T, bout, layer, layer == layers - 1, p_tail, cid + 3)
            x, a = out[0], out[-1]
        lanes_last = x_t.mT
        x_prev = finish(x, lanes_last.reshape(-1, lanes_last.shape[-1]), alpha_bar, cid + 4)
        return x_prev.reshape(lanes_last.shape).mT

    return jax.shard_map(local_step, mesh=mesh, in_specs=in_specs, out_specs=part_spec, check_vma=False)
```

```python
import functools
import math

import jax
import jax.numpy as jnp
from jax import lax
from jax.experimental import pallas as pl
from jax.experimental.pallas import tpu as pltpu
from jax.sharding import PartitionSpec as P

GUIDANCE = 4.5
LN_EPS = 1e-6
HD = 72
NH = 4
TP = 4
F32 = jnp.float32
BF16 = jnp.bfloat16
QK_SCALE = HD ** -0.5
QK_EXP2 = QK_SCALE * math.log2(math.e)
SAFE_EXP2 = 48.0
SAFE_V = 1e12
VMEM = 62914560
HBM = pl.BlockSpec(memory_space=pltpu.HBM)
MESH = pl.DeviceIdType.MESH
DOWN, ALONG = [dict(axis=axis, keepdims=True) for axis in range(2)]
PROJ, CQ, CPROJ, FC1, FC2A, FC2B = WEIGHTS = range(6)
SMALL = (PROJ, CQ, CPROJ)
PLACES = ('own', 'near', 'far_a', 'far_b', 'rest_a', 'rest_b')


def dot(a, b, dims='nn'):
    dims = {'nn': ((1,), (0,)), 'nt': ((1,), (1,)), 'tn': ((0,), (0,))}[dims]
    return lax.dot_general(a, b, (dims, ((), ())), preferred_element_type=F32)


def mod_row(refs, i):
    table, block, final, embed = refs
    layer, i = divmod(i, table.shape[1])
    d = table.shape[2]
    if layer < table.shape[0]:
        return table[layer].astype(F32)[i:i + 1] + block[...].astype(F32)[:, i * d:(i + 1) * d]
    return final[...].astype(F32)[i:i + 1] + embed[...].astype(F32)


def layer_norm(values):
    mean_val = jnp.mean(values, **ALONG)
    centered = values - mean_val
    variance = jnp.mean(centered * centered, **ALONG)
    return centered * lax.rsqrt(variance + LN_EPS)


def where_am_i():
    t, y = lax.axis_index('tp'), lax.axis_index('cfg')
    return t, y, lax.rem(t, 2)


def target(kind):
    t, y, c = where_am_i()
    return {
        'core': {'tp': t + 1 - 2 * c, 'cfg': y},
        'x': {'tp': lax.rem(t + 2, 4), 'cfg': y},
        'diag': {'tp': 3 - t, 'cfg': y},
        'y': {'tp': t, 'cfg': 1 - y},
    }[kind]


def guarded(cond, fn):
    if cond == 'all':
        fn()
        return
    _, y, c = where_am_i()
    pl.when(c == y if cond == 'same' else c != y)(fn)


def receiver(kind, cond):
    if cond == 'all' or kind in ('x', 'diag'):
        return cond
    return 'diff' if cond == 'same' else 'same'


def greet():
    barrier = pltpu.get_barrier_semaphore()
    for kind in ('core', 'x', 'diag', 'y'):
        pl.semaphore_signal(barrier, inc=1, device_id=target(kind), device_id_type=MESH)
    pl.semaphore_wait(barrier, 4)


class Comm:
    def __init__(self, ops, refs, sems):
        self.ops, self.refs, self.sems = ops, refs, sems
        self.left = {op[1] for op in ops}

    def descriptor(self, i):
        src, dst, kind, cond = self.ops[i]
        return pltpu.make_async_remote_copy(
            src_ref=self.refs[src], dst_ref=self.refs[dst], send_sem=self.sems.at[0, i], recv_sem=self.sems.at[1, i],
            device_id=target(kind), device_id_type=MESH)

    def start(self, ops):
        for i, op in enumerate(self.ops):
            if op in ops:
                guarded(op[3], lambda: self.descriptor(i).start())

    def arrive(self, name):
        if name in self.left:
            self.left.remove(name)
            i = [op[1] for op in self.ops].index(name)
            guarded(receiver(*self.ops[i][2:]), lambda: self.descriptor(i).wait_recv())

    def finish(self):
        for i, op in enumerate(self.ops):
            guarded(op[3], lambda: self.descriptor(i).wait_send())
            self.arrive(op[1])


class Buffers:
    def __init__(self):
        self.arrays = {}

    def put(self, name, array, shape=(), index=()):
        self.arrays[name] = array, shape or array.shape, index

    def take(self, made, outs):
        for name, array in zip(made, outs):
            self.put(name, array)

    def plan(self, ops):
        made = [op[1] for op in ops]
        read = []
        for op in ops:
            if op[0] not in made and op[0] not in read:
                read.append(op[0])
        return read, made

    def shape(self, name, ops):
        for src, dst, _, _ in ops:
            if dst == name:
                return self.shape(src, ops)
        return self.arrays[name][1]

    def operands(self, names):
        return [self.arrays[n][0] for n in names]

    def bind(self, read, made, in_refs, out_refs):
        refs = {}
        for n, ref in zip(read, in_refs):
            index = self.arrays[n][2]
            refs[n] = ref.at[index] if index else ref
        refs.update(zip(made, out_refs))
        return refs


def comm_params(cid, n_ops):
    return dict(
        sems=pltpu.SemaphoreType.DMA((2, n_ops)),
        params=pltpu.CompilerParams(vmem_limit_bytes=VMEM, collective_id=cid, has_side_effects=True),
    )


HALVES = ('a00', 'a01', 'a10', 'a11', 'a20', 'a30', 'a21', 'a31')
TIGHT = HALVES[4:]


def qkv(bufs, x, mods, w_rows, w_heads, layer, gather, ops, cid):
    d = x.shape[1]
    n = x.shape[0] * (TP if gather else 1)
    blk = n // len(HALVES)
    piece = NH * HD
    moves = []
    if gather:
        bufs.put('mid', x, (blk // 2, d), (slice(blk // 2, blk),))
        bufs.put('high', x, (blk, d), (slice(blk, 2 * blk),))
        moves = [('mid', 'a2m', 'x', 'all'), ('high', 'a2h', 'x', 'all'), ('a', 'a1', 'core', 'all'),
                 ('a2l', 'a3l', 'core', 'all'), ('a2m', 'a3m', 'core', 'all'), ('a2h', 'a3h', 'core', 'all')]
    late = moves[4:]
    all_ops = moves + ops
    bufs.put('a', x)
    read, made = bufs.plan(all_ops)
    read = ['a'] + [name for name in read if name != 'a']
    n_in = 3 + len(read)

    def body(*refs):
        mod_refs, refs = refs[:4], refs[4:]
        wq_ref, wk_ref, wv_ref = refs[:3]
        q_ref, k_ref, v_ref, n_ref = refs[n_in:n_in + 4]
        named = bufs.bind(read, made, refs[3:n_in], refs[n_in + 4:n_in + 4 + len(made)])
        xbuf, wqv, wk, lsem, sems = refs[n_in + 4 + len(made):]
        comm = Comm(all_ops, named, sems)
        step = pl.program_id(0)
        t, y, c = where_am_i()
        owners = [t, t + 1 - 2 * c, lax.rem(t + 2, 4), 3 - t]

        def sources(s):
            r, half = [int(digit) for digit in HALVES[s][1:]]
            if not gather:
                return [named['a'].at[pl.ds(owners[r] * 2 * blk + half * blk, blk)]]
            if r < 2:
                return [named[('a', 'a1')[r]].at[half * blk:half * blk + blk]]
            return [named['a%d%s' % (r, part)] for part in ('h' if half else 'lm')]

        def load(s):
            copies, at = [], 0
            for i, src in enumerate(sources(s)):
                dst = xbuf.at[s % 2, at:at + src.shape[0]]
                copies.append(pltpu.make_async_copy(src, dst, lsem.at[s % 2, i]))
                at += src.shape[0]
            return copies

        def begin(s):
            for name in {'a10': ('a1',), 'a20': ('a2m',), 'a30': ('a3l', 'a3m'), 'a21': ('a2h',), 'a31': ('a3h',)}.get(HALVES[s], ()):
                comm.arrive(name)
            for cp in load(s):
                cp.start()

        for s in range(len(HALVES)):
            @pl.when(step == s)
            def _():
                if s == 0:
                    begin(s)
                    greet()
                    comm.start([op for op in all_ops if op not in late])
                    wqv[0:piece] = wq_ref[...]
                    wqv[piece:2 * piece] = wv_ref[...]
                    for h in range(NH):
                        head = jnp.concatenate([wk_ref[h].astype(F32), jnp.zeros((128 - HD, d), F32)])
                        wk[h * 128:(h + 1) * 128] = head.astype(BF16)
                if gather and HALVES[s] in TIGHT:
                    begin(s)
                    comm.start([op for op in late if op[0] == {'a20': 'a2m', 'a21': 'a2h'}.get(HALVES[s])])
                for cp in load(s):
                    cp.wait()
                for name in HALVES[s + 1:s + 2]:
                    if not gather or name not in TIGHT:
                        begin(s + 1)

        x = xbuf[lax.rem(step, 2)]
        a = x
        if not gather:
            shift, scale = [mod_row(mod_refs, 6 * layer + i) for i in range(2)]
            a = (layer_norm(x.astype(F32)) * (1.0 + scale) + shift).astype(BF16)
        qv = dot(wqv[...], a, 'nt')
        q, v = qv[:piece], qv[piece:]
        norms = []
        for h in range(NH):
            qh = q[h * HD:(h + 1) * HD].astype(BF16).astype(F32)
            q_ref[h] = jnp.concatenate([qh, jnp.zeros((128 - HD, blk), F32)]).astype(BF16)
            norms.append(jnp.max(jnp.sum(qh * qh, **DOWN), **ALONG))
        kb = dot(a, wk[...], 'nt').astype(BF16)
        k_ref[...] = kb
        for h in range(NH):
            kh = kb[:, h * 128:(h + 1) * 128].astype(F32)
            norms.append(jnp.max(jnp.sum(kh * kh, **ALONG), **DOWN))
        for h in range(NH):
            v_ref[h] = v[h * HD:(h + 1) * HD].astype(BF16)
        norms.append(jnp.max(jnp.max(jnp.abs(v), **DOWN), **ALONG))
        n_ref[0] = jnp.concatenate([jnp.broadcast_to(m, (1, 128)) for m in norms] + [jnp.zeros((7, 128), F32)])

        @pl.when(step == len(HALVES) - 1)
        def _():
            comm.finish()

    def block(i):
        return i + jnp.where(i == 5, 1, 0) - jnp.where(i == 6, 1, 0)

    extra = comm_params(cid, len(all_ops))
    out = pl.pallas_call(
        body,
        grid=(len(HALVES),),
        in_specs=[pl.BlockSpec(memory_space=pltpu.VMEM)] * len(mods) + [
            pl.BlockSpec((None, None, piece, d), lambda i: (layer, 0, 0, 0)),
            pl.BlockSpec((None, None, NH, HD, d), lambda i: (layer, 1, 0, 0, 0)),
            pl.BlockSpec((None, None, piece, d), lambda i: (layer, 2, 0, 0)),
        ] + [HBM] * len(read),
        out_specs=[
            pl.BlockSpec((NH, 128, blk), lambda i: (0, 0, block(i))),
            pl.BlockSpec((blk, NH * 128), lambda i: (block(i), 0)),
            pl.BlockSpec((NH, HD, blk), lambda i: (0, 0, block(i))),
            pl.BlockSpec((1, 16, 128), lambda i: (i, 0, 0)),
        ] + [HBM] * len(made),
        out_shape=[
            jax.ShapeDtypeStruct((NH, 128, n), BF16),
            jax.ShapeDtypeStruct((n, NH * 128), BF16),
            jax.ShapeDtypeStruct((NH, HD, n), BF16),
            jax.ShapeDtypeStruct((len(HALVES), 16, 128), F32),
        ] + [jax.ShapeDtypeStruct(bufs.shape(m, all_ops), BF16) for m in made],
        scratch_shapes=[
            pltpu.VMEM((2, blk, d), BF16), pltpu.VMEM((2 * piece, d), BF16), pltpu.VMEM((NH * 128, d), BF16),
            pltpu.SemaphoreType.DMA((2, 2)), extra['sems'],
        ],
        compiler_params=extra['params'],
        name='qkv_%d' % cid,
    )(*mods, w_rows, w_heads, w_rows, *bufs.operands(read))
    bufs.take(made, out[4:])
    return out[:4]


def attention(bufs, q, k, v, first, ops, cid, bq=512, bk=1024):
    n = k.shape[0]
    own = n // TP
    per = own // bq
    read, made = bufs.plan(ops)
    steps = (NH, 2 * per)

    def body(*refs):
        q_ref, k_ref, v_ref = refs[:3]
        o_ref = refs[3 + len(read)]
        named = bufs.bind(read, made, refs[3:3 + len(read)], refs[4 + len(read):4 + len(read) + len(made)])
        comm = Comm(ops, named, refs[-1])
        head, block = pl.program_id(0), pl.program_id(1)

        @pl.when((head == 0) & (block == 0))
        def _():
            greet()
            comm.start(ops)

        def score(j):
            return dot(k_ref[j * bk:(j + 1) * bk], q_ref[0])

        s = score(0)
        total = jnp.zeros((8, bq), F32)
        acc = jnp.zeros((HD, bq), F32)
        for j in range(n // bk):
            if j + 1 < n // bk:
                ahead = score(j + 1)
            p = jnp.exp2(s * QK_EXP2)
            part = jnp.sum(p.reshape(bk // 8, 8, bq), axis=0)
            mix = dot(v_ref[0, :, j * bk:(j + 1) * bk], p.astype(BF16))
            total, acc = total + part, acc + mix
            s = ahead
        o_ref[0, 0] = (acc / jnp.sum(total, **DOWN)).astype(BF16)

        @pl.when((head == steps[0] - 1) & (block == steps[1] - 1))
        def _():
            comm.finish()

    extra = comm_params(cid, len(ops))
    out = pl.pallas_call(
        body,
        grid=steps,
        in_specs=[
            pl.BlockSpec((1, 128, bq), lambda h, i: (h, 0, first * per + i)),
            pl.BlockSpec((n, 128), lambda h, i: (0, h)),
            pl.BlockSpec((1, HD, n), lambda h, i: (h, 0, 0)),
        ] + [HBM] * len(read),
        out_specs=[pl.BlockSpec((1, 1, HD, bq), lambda h, i: (i // per, h, 0, i % per))] + [HBM] * len(made),
        out_shape=[jax.ShapeDtypeStruct((2, NH, HD, own), BF16)]
        + [jax.ShapeDtypeStruct(bufs.shape(m, ops), BF16) for m in made],
        scratch_shapes=[extra['sems']],
        compiler_params=extra['params'],
        name='attn_%d' % cid,
    )(q, k, v, *bufs.operands(read))
    bufs.take(made, out[1:])
    return out[0]


def repair_body(n_ref, q_hbm, k_hbm, v_hbm, o_hbm, out_hbm, q_ref, k_ref, v_ref, o_ref, sems, *, first):
    big = jnp.max(n_ref[...], axis=0)
    bound = jnp.max(jnp.sqrt(big[0:4]) * jnp.sqrt(big[4:8])) * QK_EXP2
    own = o_hbm.shape[3]
    bq = q_ref.shape[1]
    n = k_ref.shape[0]

    @pl.when(jnp.logical_not((bound < SAFE_EXP2) & (jnp.max(big[8:9]) < SAFE_V)))
    def _():
        @pl.loop(0, NH)
        def _(h):
            col = pl.multiple_of(h * 128, 128)
            ins = [pltpu.make_async_copy(k_hbm.at[:, pl.ds(col, 128)], k_ref, sems.at[0]),
                   pltpu.make_async_copy(v_hbm.at[h], v_ref, sems.at[1])]
            for cp in ins:
                cp.start()
            for cp in ins:
                cp.wait()

            @pl.loop(0, 2 * own // bq)
            def _(i):
                cp = pltpu.make_async_copy(q_hbm.at[h, :, pl.ds(pl.multiple_of(first * own + i * bq, bq), bq)], q_ref, sems.at[2])
                cp.start()
                cp.wait()

                def step(j, carry):
                    top, total, acc = carry
                    row = pl.multiple_of(j * bq, bq)
                    s = dot(k_ref[pl.ds(row, bq)], q_ref[...])
                    high = jnp.maximum(top, jnp.max(s, **DOWN))
                    p = jnp.exp2((s - high) * QK_EXP2)
                    shrink = jnp.exp2((top - high) * QK_EXP2)
                    mix = dot(v_ref[:, pl.ds(row, bq)], p.astype(BF16))
                    return high, total * shrink + jnp.sum(p, **DOWN), acc * shrink + mix

                start = (jnp.full((1, bq), -3e38, F32), jnp.zeros((1, bq), F32), jnp.zeros((HD, bq), F32))
                _, total, acc = lax.fori_loop(0, n // bq, step, start)
                o_ref[...] = (acc / total).astype(BF16)
                dst = out_hbm.at[i // (own // bq), h, :, pl.ds(pl.multiple_of((i % (own // bq)) * bq, bq), bq)]
                cp = pltpu.make_async_copy(o_ref, dst, sems.at[3])
                cp.start()
                cp.wait()


def repair(norms, q, k, v, o, first, bq=256):
    n = k.shape[0]
    return pl.pallas_call(
        functools.partial(repair_body, first=first),
        in_specs=[pl.BlockSpec(memory_space=pltpu.VMEM)] + [HBM] * 4,
        out_specs=HBM,
        out_shape=jax.ShapeDtypeStruct(o.shape, o.dtype),
        scratch_shapes=[
            pltpu.VMEM((128, bq), BF16), pltpu.VMEM((n, 128), BF16), pltpu.VMEM((HD, n), BF16), pltpu.VMEM((HD, bq), BF16),
            pltpu.SemaphoreType.DMA((4,)),
        ],
        input_output_aliases={4: 0},
        compiler_params=pltpu.CompilerParams(vmem_limit_bytes=VMEM),
        name='repair',
    )(norms, q, k, v, o)


def tail(bufs, cap_len, x, o_own, o_far, o_rest, mods, cross, w_out, b_out, layer, last, plan, cid, bt=256, bs=512):
    d = x.shape[1]
    n = o_own.shape[2]
    piece = NH * HD
    ops = [('o1', 'o1_in', 'core', 'all')] + sum(plan, [])
    bufs.put('low', x, (bt, d))
    made = [op[1] for op in ops[1:]]
    read = [m for m in [(p, layer, w) for p in PLACES for w in WEIGHTS] if m not in made]
    read += [op[0] for op in sum(plan[:3], []) if op[0] not in read + made]
    n_vmem = 7
    n_in = n_vmem + 4 + len(read)
    n_out = 1 if last else 2

    def body(*refs):
        mod_refs, refs = refs[:4], refs[4:]
        s_ref, c0, c1, c2, c3, wout_ref, bout_ref, x_hbm, oo, of, orr = refs[:n_vmem + 4]
        outs = refs[n_in:n_in + n_out]
        named = bufs.bind(read, made, refs[n_vmem + 4:n_in], refs[n_in + n_out:n_in + n_out + len(made)])
        scratch = refs[n_in + n_out + len(made):]
        xs, ms, os, wp, wcq, wcp, w1, w2, part, heads, lsem, osem, sems = scratch[:13]
        x_in = xs if last else scratch[13]
        named['o1'] = oo.at[1]
        named['o1_in'] = os.at[piece:2 * piece]
        if not last:
            named['low'] = outs[1].at[0:bt]
        comm = Comm(ops, named, sems)
        c_refs = (c0, c1, c2, c3)

        def place(w, r):
            if w in SMALL:
                return (wp, wcq, wcp)[w].at[r * piece:(r + 1) * piece]
            low = r % 2 * d
            if w == FC1:
                return w1.at[r // 2, :, low:low + d]
            low = r * d + d // 2 * (w == FC2B)
            return w2.at[low:low + d // 2]

        def copy(name, w, r):
            return pltpu.make_async_copy(named[(name, layer, w)], place(w, r), lsem.at[w, r])

        def fetch(w, r):
            if r < 2:
                copy(PLACES[r], w, r).start()
                return
            for cond, name in zip(('same', 'diff'), PLACES[2 * r - 2:2 * r]):
                comm.arrive((name, layer, w))
                guarded(cond, copy(name, w, r).start)

        def ready(w, r):
            copy(PLACES[0], w, r).wait()

        t, _, _ = where_am_i()
        x_from = x_hbm if last else x_hbm.at[pl.ds(t * n, n)]
        pieces = [(oo.at[0], os.at[0:piece]), (of, os.at[2 * piece:3 * piece]), (orr, os.at[3 * piece:4 * piece]), (x_from, x_in)]
        loads = [pltpu.make_async_copy(src, dst, osem.at[i, 0]) for i, (src, dst) in enumerate(pieces)]
        for cp in loads:
            cp.start()
        here = [(w, r) for w in SMALL for r in range(TP) if r < 2 or (PLACES[2 * r - 2], layer, w) not in made]
        for w, r in here:
            fetch(w, r)
        greet()
        comm.start(ops[:1] + plan[0])
        for w in SMALL:
            for r in range(TP):
                if (w, r) not in here:
                    fetch(w, r)
        for cp in loads:
            cp.wait()
        comm.arrive('o1_in')
        for w in (FC1, FC2A, FC2B):
            for r in range(2):
                fetch(w, r)

        gate1, shift2, scale2, gate2, shift3, scale3 = [mod_row(mod_refs, 6 * layer + i) for i in range(2, 8)]
        keys = lax.broadcasted_iota(jnp.int32, (128, bs), 0) < s_ref[0]

        @pl.loop(0, n // bs)
        def _(b):
            rows = pl.ds(pl.multiple_of(b * bs, bs), bs)

            def first(w):
                @pl.when(b == 0)
                def _():
                    for r in range(TP):
                        ready(w, r)

            first(PROJ)
            y = dot(os[:, rows], wp[...], 'tn')
            x = x_in[rows, :].astype(F32) + gate1 * y.astype(BF16).astype(F32)
            first(CQ)

            @pl.when(b == n // bs - 1)
            def _():
                for op in plan[1]:
                    comm.arrive(op[0])
                comm.start(plan[1])

            q = dot(wcq[...], x.astype(BF16), 'nt')
            for r in range(TP):
                scores = []
                for h in range(NH):
                    row = (r * NH + h) * HD
                    s = dot(c_refs[r][h], q[row:row + HD].astype(BF16), 'tn') * QK_SCALE
                    scores.append(jnp.where(keys, s, -1e30))
                probs = [jnp.exp(s - jnp.max(s, **DOWN)) for s in scores]
                totals = [jnp.sum(p, **DOWN) for p in probs]
                mixes = [dot(c_refs[r][NH + h], probs[h].astype(BF16)) for h in range(NH)]
                mixes = [m / total for m, total in zip(mixes, totals)]
                heads[r * piece:(r + 1) * piece] = jnp.concatenate(mixes).astype(BF16)
            first(CPROJ)
            z = dot(heads[...], wcp[...], 'tn')
            x = x + z.astype(BF16).astype(F32)
            xs[rows, :] = x
            ms[rows, :] = (layer_norm(x) * (1.0 + scale2) + shift2).astype(BF16)

        for r in range(2, TP):
            fetch(FC1, r)
            fetch(FC2A, r)

        def store(b):
            rows = pl.ds(pl.multiple_of(b * bt, bt), bt)
            return [pltpu.make_async_copy(v.at[rows], out.at[rows], osem.at[TP + i, b]) for i, (v, out) in enumerate(zip((xs, ms), outs))]

        cut = 512
        cuts = [(lo, min(lo + cut, 2 * d)) for lo in range(0, 2 * d, cut)]

        blocks = n // bt

        @pl.loop(0, 2 * blocks)
        def _(i):
            pair, b = i // blocks, i % blocks
            for p in range(2):
                @pl.when(i == p * blocks)
                def _():
                    for w in (FC1, FC2A, FC2B):
                        for r in range(2):
                            ready(w, 2 * p + r)

            rows = pl.ds(pl.multiple_of(b * bt, bt), bt)
            m = ms[rows, :]

            def up(j):
                return dot(m, w1[pair, :, cuts[j][0]:cuts[j][1]])

            u, add = up(0), jnp.zeros((bt, d), F32)
            for j, (lo, hi) in enumerate(cuts):
                if hi < 2 * d:
                    ahead = up(j + 1)
                half = 0.5 * u
                g = half + half * jnp.tanh(u * (GELU0 + GELU1 * (u * u)))
                add += dot(g.astype(BF16), w2[pl.ds(pl.multiple_of(pair * 2 * d + lo, 256), hi - lo), :])
                u = ahead

            @pl.when(pair == 0)
            def _():
                part[rows, :] = add

            @pl.when(i == blocks - 1)
            def _():
                for op in plan[2]:
                    comm.arrive(op[0])
                comm.start(plan[2])
                for r in range(2, TP):
                    fetch(FC2B, r)

            @pl.when(pair == 1)
            def _():
                x = xs[rows, :] + gate2 * (part[rows, :] + add).astype(BF16).astype(F32)
                a = (layer_norm(x) * (1.0 + scale3) + shift3).astype(BF16)
                if last:
                    outs[0][:, rows] = dot(wout_ref[...], a, 'nt') + bout_ref[:, 0:1]
                else:
                    xs[rows, :] = x
                    ms[rows, :] = a
                    for cp in store(b):
                        cp.start()

            if plan[3]:
                @pl.when(i == blocks)
                def _():
                    store(0)[1].wait()
                    comm.start(plan[3])

        if not last:
            for cp in sum([store(b) for b in range(1, blocks)], store(0)[:1]):
                cp.wait()
        comm.finish()

    vm = pl.BlockSpec(memory_space=pltpu.VMEM)
    results = [jax.ShapeDtypeStruct((w_out.shape[0], n), F32)]
    if not last:
        results = [jax.ShapeDtypeStruct((n, d), dtype) for dtype in (F32, BF16)]
    extra = comm_params(cid, len(ops))
    square = pltpu.VMEM((d, d), BF16)
    of_layer = pl.BlockSpec((None, *cross[0].shape[1:]), lambda i: (layer, 0, 0, 0))
    out = pl.pallas_call(
        body,
        grid=(1,),
        in_specs=[vm] * len(mods) + [pl.BlockSpec(memory_space=pltpu.SMEM), of_layer] + [vm] * (TP + 1) + [HBM] * (4 + len(read)),
        out_specs=[vm if last else HBM] * n_out + [HBM] * len(made),
        out_shape=results + [jax.ShapeDtypeStruct(bufs.shape(m, ops), BF16) for m in made],
        scratch_shapes=[
            pltpu.VMEM((n, d), F32), pltpu.VMEM((n, d), BF16), pltpu.VMEM((d, n), BF16), square, square, square, pltpu.VMEM((2, d, 2 * d), BF16), pltpu.VMEM((TP * d, d), BF16), pltpu.VMEM((n, d), F32), pltpu.VMEM((d, bs), BF16),
            pltpu.SemaphoreType.DMA((len(WEIGHTS), TP)), pltpu.SemaphoreType.DMA((TP + 2, n // bt)), extra['sems'],
        ] + [pltpu.VMEM((n, d), BF16)] * (not last),
        compiler_params=extra['params'],
        name='tail_%d' % cid,
    )(*mods, cap_len, *cross, w_out, b_out, x, o_own, o_far, o_rest, *bufs.operands(read))
    bufs.take(made, out[n_out:])
    return out[:n_out]


def split3(v):
    high = v.astype(BF16)
    rest = v - high.astype(F32)
    mid = rest.astype(BF16)
    return high, mid, (rest - mid.astype(F32)).astype(BF16)


def finish(tokens, x_t, alpha_bar, cid):
    total, lanes = x_t.shape
    own = total // TP
    peers = ('core', 'x', 'diag')

    def body(tok_ref, x_ref, ab_ref, out_ref, mine, other, sems):
        t, y, _ = where_am_i()
        greet()
        cols = lax.broadcasted_iota(jnp.int32, (lanes, 2 * lanes), 1)
        twice = 2 * lax.broadcasted_iota(jnp.int32, (lanes, 2 * lanes), 0)
        terms = []
        for q in range(2):
            rows = [tok_ref[16 * p + 8 * q:16 * p + 8 * q + 8, k * lanes:(k + 1) * lanes] for k in range(8) for p in range(2)]
            pick = (cols == twice + q).astype(F32).astype(BF16)
            for part in split3(jnp.concatenate(rows)):
                terms.append(dot(part, pick))
        wide = sum(terms[1:], terms[0])
        for k in range(8):
            for odd in range(2):
                half = wide[16 * k:16 * k + 16, odd * lanes:(odd + 1) * lanes]
                mine[16 * k + 8 * odd:16 * k + 8 * odd + 8] = jnp.concatenate([half[0:4], half[8:12]])
        swap = pltpu.make_async_remote_copy(
            src_ref=mine, dst_ref=other, send_sem=sems.at[0, 3], recv_sem=sems.at[1, 3],
            device_id=target('y'), device_id_type=MESH)
        swap.start()
        swap.wait()
        first, pair = y == 0, (mine[...], other[...])
        cond, uncond = jnp.where(first, *pair), jnp.where(first, *pair[::-1])
        guided = uncond + GUIDANCE * (cond - uncond)
        abar_t, abar_prev = ab_ref[:, :1], ab_ref[:, 1:]
        rows = pl.ds(pl.multiple_of(t * own, own), own)
        x_zero = (x_ref[rows] - jnp.sqrt(1.0 - abar_t) * guided) / jnp.sqrt(abar_t)
        out_ref[rows] = jnp.sqrt(abar_prev) * x_zero + jnp.sqrt(1.0 - abar_prev) * guided
        sends = [pltpu.make_async_remote_copy(
            src_ref=out_ref.at[rows], dst_ref=out_ref.at[rows], send_sem=sems.at[0, i], recv_sem=sems.at[1, i],
            device_id=target(kind), device_id_type=MESH) for i, kind in enumerate(peers)]
        for cp in sends:
            cp.start()
        for cp in sends:
            cp.wait()

    vm = pl.BlockSpec(memory_space=pltpu.VMEM)
    return pl.pallas_call(
        body,
        in_specs=[vm] * 3,
        out_specs=vm,
        out_shape=jax.ShapeDtypeStruct(x_t.shape, F32),
        scratch_shapes=[pltpu.VMEM((own, lanes), F32)] * 2 + [pltpu.SemaphoreType.DMA((2, 4))],
        compiler_params=pltpu.CompilerParams(collective_id=cid, has_side_effects=True),
        name='finish',
    )(tokens, x_t, alpha_bar)


GELU0 = math.sqrt(2.0 / math.pi)
GELU1 = GELU0 * 0.044715


def over_x(layer, ws):
    return [(('own', layer, w), ('far_a', layer, w), 'x', 'same') for w in ws]


def to_core(layer, ws):
    return [(('own', layer, w), ('near', layer, w), 'core', 'all') for w in ws]


def forward(layer, ws):
    return [op for w in ws for op in (
        (('far_a', layer, w), ('far_b', layer, w), 'y', 'same'), (('far_a', layer, w), ('rest_b', layer, w), 'core', 'same'))]


def hand_on(layer, ws):
    return [(('far_b', layer, w), ('rest_a', layer, w), 'core', 'diff') for w in ws]


def share(layer):
    return [(('c', 0, layer), ('c', r, layer), kind, 'all') for r, kind in ((1, 'core'), (2, 'x'))]


def share_on(layer):
    return [(('c', 2, layer), ('c', 3, layer), 'core', 'all')]


def solution(mesh):
    row_spec = P(('dp', 'cfg'))
    part_spec = P('dp')
    tp1, tp2, tp3 = [P(*(None,) * i, 'tp') for i in range(1, 4)]
    in_specs = (row_spec, row_spec, row_spec, part_spec, part_spec, part_spec, part_spec, P(),
                tp3, tp1, tp2, tp3, tp1, tp2, tp1, P(), P(), P())

    def local_step(hidden, caption, cap_len, t_block, t_embed, x_t, alpha_bar, mod_table, w_qkv, w_proj, w_cq, w_ckv, w_cproj, w_fc1, w_fc2, final_table, w_out, b_out):
        n, d = hidden.shape[1:]
        own_n = n // TP
        layers = mod_table.shape[0]

        w_heads = w_qkv.transpose(0, 2, 3, 4, 1)
        w_rows = w_heads.reshape(layers, 3, NH * HD, d)
        by_rows = lambda w: w.reshape(layers, NH * HD, d)
        owned = (by_rows(w_proj), by_rows(w_cq.transpose(0, 2, 3, 1)), by_rows(w_cproj), w_fc1)
        bufs = Buffers()
        for layer in range(layers):
            for w, array in enumerate(owned):
                bufs.put(('own', layer, w), array, array.shape[1:], (layer,))
            for half in range(2):
                index = (layer, slice(half * d // 2, (half + 1) * d // 2))
                bufs.put(('own', layer, FC2A + half), w_fc2, (d // 2, d), index)

        mods = (mod_table, t_block, final_table, t_embed)
        bout = jnp.broadcast_to(b_out.astype(F32)[:, None], (b_out.shape[0], 128))

        cap = jnp.pad(caption[0], ((0, 128 - caption.shape[1]), (0, 0)))
        ckv_t = w_ckv.transpose(0, 2, 3, 4, 1).reshape(layers * 2 * NH * HD, d)
        ckv = dot(ckv_t, cap, 'nt').astype(BF16).reshape(layers, 2 * NH, HD, 128)
        for layer in range(layers):
            bufs.put(('c', 0, layer), ckv, ckv.shape[1:], (layer,))

        plans = [
            (to_core(0, WEIGHTS) + over_x(0, SMALL) + share(0),
             over_x(0, [FC1]) + over_x(1, [PROJ]) + forward(0, SMALL) + share_on(0),
             over_x(0, [FC2A]) + forward(0, [FC1]) + forward(1, [PROJ]) + hand_on(0, SMALL),
             (over_x(0, [FC2B]) + forward(0, [FC2A]) + hand_on(0, [FC1]) + hand_on(1, [PROJ]) + over_x(1, [FC1]) + to_core(1, WEIGHTS),
              forward(0, [FC2B]) + hand_on(0, [FC2A]), hand_on(0, [FC2B]),
              [('low', 'a2l', 'x', 'all')])),
            (forward(1, [FC1]),
             over_x(1, [CQ, CPROJ, FC2A]) + hand_on(1, [FC1]) + share(1),
             forward(1, [CQ, CPROJ, FC2A]) + share_on(1),
             (hand_on(1, [CQ, CPROJ, FC2A]) + over_x(1, [FC2B]), forward(1, [FC2B]), hand_on(1, [FC2B]), [])),
        ]
        x = a = hidden[0]
        for layer in range(layers):
            p_qkv, p_other, p_own, p_tail = plans[layer]
            cid = 1 + 4 * layer
            q, k, v, norms = qkv(bufs, a, mods, w_rows, w_heads, layer, layer > 0, p_qkv, cid)
            o = attention(bufs, q, k, v, 2, p_other, cid + 1)
            o = repair(norms, q, k, v, o, 2).reshape(2, NH * HD, own_n)
            for i in range(2):
                bufs.put(('o', layer, i), o, o.shape[1:], (i,))
            send = [(('o', layer, i), ('o_in', layer, i), kind, 'all') for i, kind in enumerate(('x', 'diag'))]
            o = attention(bufs, q, k, v, 0, send + p_own, cid + 2)
            o = repair(norms, q, k, v, o, 0).reshape(2, NH * HD, own_n)
            o_far, o_rest = [bufs.arrays[('o_in', layer, i)][0] for i in range(2)]
            cross = [bufs.arrays[('c', r, layer)][0] for r in range(TP)]
            out = tail(bufs, cap_len, x, o, o_far, o_rest, mods, cross, w_out.T, bout, layer, layer == layers - 1, p_tail, cid + 3)
            x, a = out[0], out[-1]
        lanes_last = x_t.mT
        x_prev = finish(x, lanes_last.reshape(-1, lanes_last.shape[-1]), alpha_bar, cid + 4)
        return x_prev.reshape(lanes_last.shape).mT

    return jax.shard_map(local_step, mesh=mesh, in_specs=in_specs, out_specs=part_spec, check_vma=False)
```
